32 devices in a mesh: tm: 8 (over y, x, core), space: 4 (over z).
Axes of the slice: x: 2, y: 2, z: 4, core: 2. Of those that a mesh axis runs over, the one named last changes fastest.
Arguments:
- initial_state: float32 [1024, 1024], P('space'), may hold values from -6 to 6
- guess_coarse: float32 [8, 1024, 1024], P('tm', 'space'), may hold values from -6 to 6
- force_fine: float32 [8, 1024, 1024], P('tm', 'space'), may hold values from -6 to 6
- force_coarse: float32 [8, 1024, 1024], P('tm', 'space'), may hold values from -6 to 6
- eigen_basis: float32 [1024, 1024], replicated, may hold values from -1 to 1, as said below
- eigen_rates: float32 [1024], replicated, may hold values from 0.02 to 4
- carried_correction: float32 [1024, 1024], replicated, may hold values from -6 to 6
Outputs:
- fine_states: float32 [8, 1024, 1024], P('tm', 'space')
- coarse_states: float32 [8, 1024, 1024], P('tm', 'space')
The draws below stay inside these ranges and needn't reach their ends.
Inputs may be any that keep to these rules, and one draw needn't show every extreme that they name: `eigen_basis`: an orthogonal matrix: its transpose is its inverse up to float32 rounding.
All inputs are finite; a program needn't handle non-finite values.
Results may differ from the reference program's by a relative error of at most 0.00013.
Values sent between devices are 32-bit elements; how exact they have to be, the bound alone decides.
A program may use at most 128 MiB of HBM per device.

```python
import math
import jax
import jax.numpy as jnp
from jax import lax

GRID = 1024
GROUPS = 8


def draw_eigen_basis(key, part):
    skewed = jax.random.normal(key, (GRID, GRID), jnp.float32) / math.sqrt(GRID)
    skewed = skewed - skewed.T
    identity = jnp.eye(GRID, dtype=jnp.float32)
    return jnp.linalg.solve(identity + skewed, identity - skewed)


def shard_levels(stream_key, dims, split, least, high):
    level = 1.0
    for dim, shards_of in split:
        heights = jax.random.uniform(jax.random.fold_in(jax.random.fold_in(stream_key, 6), dim), (shards_of,), jnp.float32, least / len(split), high / len(split))
        level = level * jnp.repeat(jnp.exp(heights), dims[dim] // shards_of).reshape((-1,) + (1,) * (len(dims) - 1 - dim))
    return level


def scatter_about(key, shape, scale, most, pieces=(), kind=jnp.bfloat16):
    loudness = shard_levels(key, shape, pieces, -0.22, 0.18) if pieces else 1.0
    array = jax.random.normal(key, shape, jnp.float32) * scale * loudness
    return jnp.minimum(jnp.maximum(array, -most), most).astype(kind)


def setup_inputs(seed: int = 0) -> dict:
    key_of = jax.random.split(jax.random.key(seed), 8)
    return {
        "initial_state": scatter_about(key_of[0], (GRID, GRID), 1.0, 6.0, ((0, 4),), jnp.float32),
        "guess_coarse": scatter_about(key_of[1], (GROUPS, GRID, GRID), 1.0, 6.0, ((0, 8), (1, 4)), jnp.float32),
        "force_fine": scatter_about(key_of[2], (GROUPS, GRID, GRID), 1.0, 6.0, ((0, 8), (1, 4)), jnp.float32),
        "force_coarse": scatter_about(key_of[3], (GROUPS, GRID, GRID), 1.0, 6.0, ((0, 8), (1, 4)), jnp.float32),
        "eigen_basis": draw_eigen_basis(jax.random.fold_in(key_of[7], 71), 0),
        "eigen_rates": jnp.clip(jnp.exp(jax.random.uniform(key_of[5], (GRID,), jnp.float32, math.log(0.02), math.log(4.0))), 0.02, 4.0),
        "carried_correction": scatter_about(key_of[6], (GRID, GRID), 1.0, 6.0, (), jnp.float32),
    }


exact_mode = lax.Precision.HIGHEST

def reference(initial_state, guess_coarse, force_fine, force_coarse, eigen_basis, eigen_rates, carried_correction):
    fine_decay = 1.0 / (1.0 + eigen_rates[:, None] + eigen_rates[None, :])
    coarse_decay = 1.0 / (1.0 + 2.0 * (eigen_rates[:, None] + eigen_rates[None, :]))

    def to_eigen(field):
        right = jnp.einsum('gij,jk->gik', field, eigen_basis, precision=exact_mode)
        return jnp.einsum('ji,gjk->gik', eigen_basis, right, precision=exact_mode)

    def from_eigen(coeffs):
        left = jnp.einsum('ij,gjk->gik', eigen_basis, coeffs, precision=exact_mode)
        return jnp.einsum('gij,kj->gik', left, eigen_basis, precision=exact_mode)

    def reaction(field):
        return field + 0.5 * jnp.tanh(field)

    def propagate(field, source):
        return from_eigen(fine_decay[None] * to_eigen(reaction(field) + source))

    def previous(states):
        return jnp.concatenate([initial_state[None], states[:-1]], axis=0)
    relaxed_fine = propagate(previous(guess_coarse), force_fine)
    relaxed_coarse = propagate(relaxed_fine, force_coarse)
    second_fine = propagate(previous(relaxed_coarse), force_fine)
    residual = fine_decay[None] * to_eigen(reaction(second_fine) + force_coarse) - to_eigen(relaxed_coarse)

    def coarse_turn(carry, term):
        updated = coarse_decay * carry + term
        return (updated, updated)
    unused, correction = lax.scan(coarse_turn, carried_correction, residual)
    coarse_states = relaxed_coarse + from_eigen(correction)
    fine_states = propagate(previous(coarse_states), force_fine)
    return (fine_states, coarse_states)
```

```python
import functools
import jax
import jax.numpy as jnp
from jax import lax
from jax.experimental import pallas as pl
from jax.experimental.pallas import tpu as pltpu
from jax.sharding import PartitionSpec as P

MESH = pl.DeviceIdType.MESH


def halves(block):
    high = block.astype(jnp.bfloat16)
    return high, (block - high.astype(jnp.float32)).astype(jnp.bfloat16)


def dot3(left, right):
    dot = functools.partial(jnp.dot, preferred_element_type=jnp.float32)
    return dot(left[0], right[0]) + dot(left[0], right[1]) + dot(left[1], right[0])


def reacted(value):
    return value + 0.5 * jnp.tanh(value)


def chain_kernel(
    raw, rates_tall, rates_wide, guess, initial, fine, coarse, basis, basis_t, terms,
    before, entry, slots, field, coeffs, kept, wide, tall, part, sent, held, decay, coarse_decay, leaving, landed,
    home_send, shift_recv, slot_recv, ex_send, ex_recv, term_send, term_recv,
):
    groups, count = lax.axis_size("tm"), lax.axis_size("space")
    t, s = lax.axis_index("tm"), lax.axis_index("space")
    grid = raw.shape[0]
    rows = fine.shape[0]
    half = grid // 2
    piece = half // 2
    per_half = count // 2
    low_seat = per_half - 1
    last = groups - 1

    def at(start, size):
        return pl.ds(pl.multiple_of(start, size), size)

    def seat(chain):
        return low_seat + chain % 2

    def core(chain, which):
        return 2 * (chain // 2) + which

    which = s // per_half
    place = at((s % per_half) * rows, rows)
    mine, past = t, (t + groups - 1) % groups
    mine_at = (core(mine, which), seat(mine))
    past_at = (core(past, which), seat(past))
    to_self = (mine_at[0] == t) & (mine_at[1] == s)

    def remote(src, dst, send, recv, where):
        return pltpu.make_async_remote_copy(
            src_ref=src, dst_ref=dst, send_sem=send, recv_sem=recv,
            device_id={"tm": where[0], "space": where[1]}, device_id_type=MESH,
        )

    def to_mine(src, slot, index):
        pos = s % per_half
        dst, recv = slots.at[slot, place], slot_recv.at[slot, pos]

        @pl.when(jnp.logical_not(to_self))
        def _():
            remote(src, dst, home_send.at[index], recv, mine_at).start()

        @pl.when(to_self)
        def _():
            pltpu.make_async_copy(src, dst, recv).start()

    def to_past(src, slot, index):
        return remote(src, slots.at[slot, place], home_send.at[index], slot_recv.at[slot, s % per_half], past_at)

    def pass_on():
        return remote(guess, before, home_send.at[4], shift_recv.at[0], ((t + 1) % groups, s))

    @pl.when(t != last)
    def _():
        pass_on().start()

    to_mine(coarse, 1, 0)

    @pl.loop(0, count)
    def _(r):
        high, low = halves(raw[at(r * rows, rows), :])
        basis[0, at(r * rows, rows), :] = high
        basis[1, at(r * rows, rows), :] = low

    @pl.when(t != 0)
    def _():
        remote(guess, before, home_send.at[4], shift_recv.at[0], (t, s)).wait_recv()
        entry[...] = reacted(before[...]) + fine[...]

    @pl.when(t == 0)
    def _():
        entry[...] = reacted(initial[...]) + fine[...]

    to_mine(entry, 0, 1)

    @pl.when(t == 0)
    def _():
        to_past(entry, 2, 2).start()

    @pl.when(t != 0)
    def _():
        to_past(fine, 2, 2).start()

    to_past(coarse, 3, 3).start()

    @pl.loop(0, grid // piece)
    def _(r):
        @pl.loop(0, grid // piece)
        def _(c):
            high, low = halves(raw[at(c * piece, piece), at(r * piece, piece)].T)
            basis_t[0, at(r * piece, piece), at(c * piece, piece)] = high
            basis_t[1, at(r * piece, piece), at(c * piece, piece)] = low

    side = t % 2
    group = 2 * (t // 2) + (s - low_seat)
    partner = (2 * (t // 2) + 1 - side, s)
    own, other = at(side * half, half), at((1 - side) * half, half)

    def wait_slot(slot, position):
        source = side * per_half + position
        dst, recv = slots.at[slot, at(position * rows, rows)], slot_recv.at[slot, position]
        local = (group == t) & (source == s) if slot < 2 else None

        def arrive():
            remote(fine, dst, home_send.at[0], recv, (t, s)).wait_recv()

        if local is None:
            arrive()
        else:
            pl.when(jnp.logical_not(local))(arrive)

            @pl.when(local)
            def _():
                pltpu.make_async_copy(fine, dst, recv).wait()

    def exchange(stage, m):
        block = at(m * piece, piece)
        return remote(sent.at[stage % 2, block], held.at[stage % 2, block], ex_send.at[stage, m], ex_recv.at[stage, m], partner)

    def collect(stage):
        for m in range(2):
            exchange(stage, m).wait_recv()
            part[0, m * piece:(m + 1) * piece, :], part[1, m * piece:(m + 1) * piece, :] = halves(
                held[stage % 2, m * piece:(m + 1) * piece, :]
            )

    def take(stage, make):
        if stage >= 2:
            for m in range(2):
                exchange(stage - 2, m).wait_send()

        @pl.loop(0, 2)
        def _(m):
            sent[stage % 2, at(m * piece, piece)] = make(m, False)
            exchange(stage, m).start()

        @pl.loop(0, 2)
        def _(m):
            block = at(m * piece, piece)
            part[0, block, :], part[1, block, :] = halves(make(m, True))

    def forward(stage, source, ready, finish):
        for m in range(per_half):
            ready(m)
            high, low = halves(source(at(m * rows, rows)))
            wide[0, at(m * rows, rows), :] = high
            wide[1, at(m * rows, rows), :] = low

        def make(m, keep):
            block, columns = at(m * piece, piece), own if keep else other
            return dot3((wide[0, block, :], wide[1, block, :]), (basis[0, :, columns], basis[1, :, columns]))

        take(stage, make)

        @pl.loop(0, grid // piece)
        def _(r):
            block = at(r * piece, piece)
            coeffs[block, :] = dot3((basis_t[0, block, own], basis_t[1, block, own]), (part[0], part[1]))

        collect(stage)

        @pl.loop(0, grid // piece)
        def _(r):
            block = at(r * piece, piece)
            term = dot3((basis_t[0, block, other], basis_t[1, block, other]), (part[0], part[1]))
            finish(r, block, (coeffs[block, :] + term) * decay[block, :])

    def inverse(stage):
        @pl.loop(0, grid // piece)
        def _(r):
            block = at(r * piece, piece)
            tall[0, block, :], tall[1, block, :] = halves(coeffs[block, :])

        def make(m, keep):
            block = at((side if keep else 1 - side) * half + m * piece, piece)
            return dot3((basis[0, block, :], basis[1, block, :]), (tall[0], tall[1]))

        take(stage, make)

        @pl.loop(0, 2)
        def _(n):
            columns = at(n * half, half)
            field[:, columns] = dot3((part[0], part[1]), (basis_t[0, own, columns], basis_t[1, own, columns]))

        collect(stage)

        @pl.loop(0, 2)
        def _(n):
            columns = at(n * half, half)
            field[:, columns] = field[:, columns] + dot3(
                (part[0], part[1]), (basis_t[0, other, columns], basis_t[1, other, columns])
            )

    @pl.when((s == low_seat) | (s == low_seat + 1))
    def _():
        @pl.loop(0, grid // piece)
        def _(r):
            block = at(r * piece, piece)
            pair = rates_tall[block, :1] + rates_wide[:1, own]
            decay[block, :] = 1.0 / (1.0 + pair)
            coarse_decay[block, :] = 1.0 / (1.0 + 2.0 * pair)

        def plain(r, block, value):
            coeffs[block, :] = value

        def keep(r, block, value):
            coeffs[block, :] = value
            kept[block, :] = jnp.where(group == last, 0.0, value * coarse_decay[block, :])

        def leave(r, block, value):
            value = value - kept[block, :]
            for q in range(per_half):
                leaving[q, block, :] = value[:, q * rows:(q + 1) * rows]
            for q in range(per_half):
                send_term(r, q)

        def term_place(q):
            return group, side * per_half + q

        def term_copy(r, q):
            block = at(r * piece, piece)
            return remote(leaving.at[q, block], landed.at[block], term_send.at[q, r], term_recv.at[r], term_place(q))

        def term_local(r, q):
            block = at(r * piece, piece)
            return pltpu.make_async_copy(leaving.at[q, block], landed.at[block], term_recv.at[r])

        def term_here(q):
            where = term_place(q)
            return (where[0] == t) & (where[1] == s)

        def send_term(r, q):
            here = term_here(q)

            @pl.when(here)
            def _():
                term_local(r, q).start()

            @pl.when(jnp.logical_not(here))
            def _():
                term_copy(r, q).start()

        def from_field(slot):
            def source(block):
                moved = reacted(field[block, :])
                if slot == 2:
                    moved = jnp.where(group == last, 0.0, moved)
                return moved + slots[slot, block, :]
            return source

        forward(0, lambda block: slots[0, block, :], lambda m: wait_slot(0, m), plain)
        inverse(1)
        forward(2, from_field(1), lambda m: wait_slot(1, m), keep)
        inverse(3)
        forward(4, from_field(2), lambda m: wait_slot(2, m), plain)
        inverse(5)
        forward(6, from_field(3), lambda m: wait_slot(3, m), leave)

        for stage in (5, 6):
            for m in range(2):
                exchange(stage, m).wait_send()
        for q in range(per_half):
            @pl.when(jnp.logical_not(term_here(q)))
            def _():
                for r in range(grid // piece):
                    term_copy(r, q).wait_send()

    term_side = s // per_half
    sender = (core(t, term_side), seat(t))
    from_self = (sender[0] == t) & (sender[1] == s)
    for r in range(grid // piece):
        block = at(r * piece, piece)

        @pl.when(from_self)
        def _():
            pltpu.make_async_copy(leaving.at[0, block], landed.at[block], term_recv.at[r]).wait()

        @pl.when(jnp.logical_not(from_self))
        def _():
            remote(leaving.at[0, block], landed.at[block], term_send.at[0, r], term_recv.at[r], (t, s)).wait_recv()

        terms[block, :] = landed[block, :]

    @pl.when(jnp.logical_not(to_self))
    def _():
        for index, src in ((0, coarse), (1, entry)):
            remote(src, slots.at[0, place], home_send.at[index], slot_recv.at[0, 0], mine_at).wait_send()

    for index in (2, 3):
        remote(fine, slots.at[0, place], home_send.at[index], slot_recv.at[0, 0], past_at).wait_send()

    @pl.when(t != last)
    def _():
        pass_on().wait_send()


def chains(basis, rates, guess, initial, fine, coarse):
    grid, rows = basis.shape[0], fine.shape[0]
    half = grid // 2
    piece, count = half // 2, grid // rows
    per_half = count // 2
    steps = 7
    f32, bf16 = jnp.float32, jnp.bfloat16
    lanes = 128
    operands = [basis, jnp.broadcast_to(rates[:, None], (grid, lanes)), rates[None, :], guess, initial, fine, coarse]
    shapes = [
        jax.ShapeDtypeStruct((2, grid, grid), bf16),
        jax.ShapeDtypeStruct((2, grid, grid), bf16),
        jax.ShapeDtypeStruct((grid, rows), f32),
    ]
    vmem = pl.BlockSpec(memory_space=pltpu.VMEM)
    dma = pltpu.SemaphoreType.DMA
    return pl.pallas_call(
        chain_kernel,
        out_shape=shapes,
        in_specs=[vmem] * len(operands),
        out_specs=[vmem] * len(shapes),
        scratch_shapes=[
            pltpu.VMEM((rows, grid), f32),
            pltpu.VMEM((rows, grid), f32),
            pltpu.VMEM((4, half, grid), f32),
            pltpu.VMEM((half, grid), f32),
            pltpu.VMEM((grid, half), f32),
            pltpu.VMEM((grid, half), f32),
            pltpu.VMEM((2, half, grid), bf16),
            pltpu.VMEM((2, grid, half), bf16),
            pltpu.VMEM((2, half, half), bf16),
            pltpu.VMEM((2, half, half), f32),
            pltpu.VMEM((2, half, half), f32),
            pltpu.VMEM((grid, half), f32),
            pltpu.VMEM((grid, half), f32),
            pltpu.VMEM((per_half, grid, rows), f32),
            pltpu.VMEM((grid, rows), f32),
            dma((5,)),
            dma((1,)),
            dma((4, per_half)),
            dma((steps, 2)),
            dma((steps, 2)),
            dma((per_half, grid // piece)),
            dma((grid // piece,)),
        ],
        compiler_params=pltpu.CompilerParams(has_side_effects=True, vmem_limit_bytes=62 * 1024 * 1024),
        cost_estimate=pl.CostEstimate(flops=150_000_000_000, bytes_accessed=16 * grid * grid, transcendentals=0),
        name="chains",
    )(*operands)


def stages_kernel(
    plan, forced, raw, basis, basis_t, spare, decay, start, sources, fixed, outs, split, split_tall, field, coeffs, sent, held, doubled, send_sem, recv_sem
):
    count = lax.axis_size("space")
    me = lax.axis_index("space")
    rows = held.shape[2]
    barrier = pltpu.get_barrier_semaphore()

    @pl.loop(0, count)
    def _(d):
        @pl.when(d != me)
        def _():
            pl.semaphore_signal(barrier, inc=1, device_id={"space": d}, device_id_type=pl.DeviceIdType.MESH)

    pl.semaphore_wait(barrier, count - 1)

    def span(d):
        return pl.ds(pl.multiple_of(d * rows, rows), rows)

    def peer(k):
        return jnp.where(me < count // 2, count - 1 - k, k)

    def copy(stage, d):
        return pltpu.make_async_remote_copy(
            src_ref=sent.at[stage, d],
            dst_ref=held.at[stage, me],
            send_sem=send_sem.at[stage, d],
            recv_sem=recv_sem.at[stage, me],
            device_id={"space": d},
            device_id_type=pl.DeviceIdType.MESH,
        )

    def arrival(stage, s):
        return pltpu.make_async_remote_copy(
            src_ref=sent.at[stage, s],
            dst_ref=held.at[stage, s],
            send_sem=send_sem.at[stage, s],
            recv_sem=recv_sem.at[stage, s],
            device_id={"space": s},
            device_id_type=pl.DeviceIdType.MESH,
        )

    def exchange(stage, block_for, use, between=None):
        @pl.loop(0, count)
        def _(k):
            d = peer(k)
            block = block_for(d)

            @pl.when(d != me)
            def _():
                sent[stage, d] = block
                copy(stage, d).start()

            @pl.when(d == me)
            def _():
                held[stage, me] = block

        if between is not None:
            between()
        use(me, True)

        @pl.loop(0, count)
        def _(k):
            s = peer(k)

            @pl.when(s != me)
            def _():
                arrival(stage, s).wait_recv()
                use(s, False)

    def split_basis():
        @pl.loop(0, count)
        def _(r):
            high, low = halves(raw[span(r), :])
            basis[0, span(r), :] = high
            basis[1, span(r), :] = low

    def turn_basis():
        @pl.loop(0, count)
        def _(r):
            @pl.loop(0, count)
            def _(c):
                high, low = halves(raw[span(c), span(r)].T)
                basis_t[0, span(r), span(c)] = high
                basis_t[1, span(r), span(c)] = low

    def forward(stage):
        high, low = halves(field[...])
        split[0] = high
        split[1] = low

        def block_for(d):
            return dot3((split[0], split[1]), (basis[0, :, span(d)], basis[1, :, span(d)]))

        def use(s, first):
            part = halves(held[stage, s])

            @pl.loop(0, count)
            def _(r):
                term = dot3((basis_t[0, span(r), span(s)], basis_t[1, span(r), span(s)]), part)
                coeffs[span(r), :] = term if first else coeffs[span(r), :] + term

        exchange(stage, block_for, use, turn_basis if raw is not None and stage == 0 else None)

    def inverse(stage):
        high, low = halves(coeffs[...])
        split_tall[0] = high
        split_tall[1] = low

        def block_for(d):
            block = dot3((basis[0, span(d), :], basis[1, span(d), :]), (split_tall[0], split_tall[1]))
            if spare is not None and stage == len(plan) - 1:
                doubled[0, span(d), :], doubled[1, span(d), :] = halves(block)
            return block

        def keep_spare():
            @pl.loop(0, count)
            def _(r):
                back = dot3((basis_t[0, span(r), :], basis_t[1, span(r), :]), (doubled[0], doubled[1]))
                spare[span(r), :] = back - coeffs[span(r), :]

        def use(s, first):
            part = halves(held[stage, s])

            @pl.loop(0, count)
            def _(r):
                term = dot3(part, (basis_t[0, span(s), span(r)], basis_t[1, span(s), span(r)]))
                field[:, span(r)] = term if first else field[:, span(r)] + term

        exchange(stage, block_for, use, keep_spare if spare is not None and stage == len(plan) - 1 else None)

    def react(source):
        value = field[...]
        field[...] = value + 0.5 * jnp.tanh(value) + source[...]

    sources = list(sources)
    outs = list(outs)
    if raw is not None:
        split_basis()
    if plan[0] == "E":
        field[...] = start[...]
        react(sources.pop(0))
    else:
        coeffs[...] = start[...]
    for stage, kind in enumerate(plan):
        final = stage == len(plan) - 1
        if kind == "E":
            forward(stage)
            coeffs[...] = coeffs[...] * decay[...]
            if stage in forced:
                outs.pop(0)[...] = coeffs[...]
        else:
            inverse(stage)
            if stage in forced:
                outs.pop(0)[...] = field[...]
            if not final:
                if fixed is not None:
                    @pl.when(lax.axis_index("tm") == lax.axis_size("tm") - 1)
                    def _():
                        field[...] = fixed[...]
                react(sources.pop(0))

    for stage in range(len(plan)):
        @pl.loop(0, count)
        def _(d):
            @pl.when(d != me)
            def _():
                copy(stage, d).wait_send()


def stages(plan, forced, number, basis, decay, start, sources, fixed=None):
    grid, rows = decay.shape
    count = grid // rows
    wide, tall = (rows, grid), (grid, rows)
    extra = 0 if fixed is None else 1
    first = not isinstance(basis, tuple)
    given = [basis] if first else list(basis)
    shapes = [jax.ShapeDtypeStruct(tall if plan[s] == "E" else wide, jnp.float32) for s in forced]
    if first:
        shapes += [jax.ShapeDtypeStruct((2, grid, grid), jnp.bfloat16)] * 2 + [jax.ShapeDtypeStruct(tall, jnp.float32)]

    def kernel(*refs):
        refs = list(refs)
        basis_refs = refs[: len(given)]
        del refs[: len(given)]
        decay_ref, start_ref = refs[:2]
        del refs[:2]
        source_refs = refs[: len(sources)]
        del refs[: len(sources)]
        fixed_ref = refs.pop(0) if extra else None
        out_refs = refs[: len(shapes)]
        raw, spare = None, None
        if first:
            raw = basis_refs[0]
            basis_refs, spare = out_refs[-3:-1], out_refs[-1]
        stages_kernel(
            plan, forced, raw, *basis_refs, spare, decay_ref, start_ref, source_refs, fixed_ref, out_refs, *refs[len(shapes):]
        )

    operands = [*given, decay, start, *sources] + ([fixed] if extra else [])
    steps = len(plan)
    vmem = pl.BlockSpec(memory_space=pltpu.VMEM)
    return pl.pallas_call(
        kernel,
        out_shape=shapes,
        in_specs=[vmem] * len(operands),
        out_specs=[vmem] * len(shapes),
        scratch_shapes=[
            pltpu.VMEM((2, *wide), jnp.bfloat16),
            pltpu.VMEM((2, *tall), jnp.bfloat16),
            pltpu.VMEM(wide, jnp.float32),
            pltpu.VMEM(tall, jnp.float32),
            pltpu.VMEM((steps, count, rows, rows), jnp.float32),
            pltpu.VMEM((steps, count, rows, rows), jnp.float32),
            pltpu.VMEM((2, *tall) if first else (2, 16, 128), jnp.bfloat16),
            pltpu.SemaphoreType.DMA((steps, count)),
            pltpu.SemaphoreType.DMA((steps, count)),
        ],
        compiler_params=pltpu.CompilerParams(
            collective_id=number, has_side_effects=True, vmem_limit_bytes=48 * 1024 * 1024
        ),
        cost_estimate=pl.CostEstimate(
            flops=steps * 40_000_000_000, bytes_accessed=8 * grid * grid, transcendentals=0
        ),
        name="stages_%d" % number,
    )(*operands)


def decay_block(eigen_rates, own_rates, factor):
    return 1.0 / (1.0 + factor * (eigen_rates[:, None] + own_rates[None, :]))


def shift(block, distance):
    count = lax.axis_size("tm")
    return lax.ppermute(block, "tm", [(i, (i + distance) % count) for i in range(count)])


def swap(block):
    count = lax.axis_size("tm")
    return lax.ppermute(block, "tm", [(i, i ^ 1) for i in range(count)])


def coarse_solve(terms, start, decay):
    count = lax.axis_size("tm")
    pairs = count // 2
    place = lax.axis_index("tm")
    pair, odd = place // 2, place % 2
    half = terms.shape[0] // 2

    def mine(block, which):
        return lax.dynamic_slice_in_dim(block, which * half, half, 0)

    other = swap(mine(terms, 1 - odd))
    own = mine(terms, odd)
    first = jnp.where(odd == 0, own, other)
    second = jnp.where(odd == 0, other, own)
    decay = mine(decay, odd)
    carried = mine(start, odd)
    is_last = pair == pairs - 1
    sums = second + decay * jnp.where(is_last, carried, first)
    squared = decay * decay
    before = jnp.where(is_last, sums, 0.0)
    arrived = {}
    for s in range(1, pairs):
        route = []
        for k in range(pairs):
            if s <= k + 1:
                source = (k - s) % pairs
                route += [(2 * source + c, 2 * k + c) for c in range(2)]
        arrived[s] = lax.ppermute(sums, "tm", route)
    for s in range(pairs - 1, 0, -1):
        before = squared * before + arrived[s]
    even_state = before
    odd_state = first + decay * even_state
    given = jnp.where(odd == 0, odd_state, even_state)
    kept = jnp.where(odd == 0, even_state, odd_state)
    got = swap(given)
    return jnp.where(
        odd == 0,
        jnp.concatenate([kept, got], 0),
        jnp.concatenate([got, kept], 0),
    )


def on_device(
    initial_state,
    guess_coarse,
    force_fine,
    force_coarse,
    eigen_basis,
    eigen_rates,
    carried_correction,
):
    row_count = initial_state.shape[0]
    offset = lax.axis_index("space") * row_count
    own_rates = lax.dynamic_slice_in_dim(eigen_rates, offset, row_count, 0)
    fine_decay = decay_block(eigen_rates, own_rates, 1.0)
    coarse_decay = decay_block(eigen_rates, own_rates, 2.0)
    carried = lax.dynamic_slice_in_dim(carried_correction, offset, row_count, 1)
    place = lax.axis_index("tm")
    basis, basis_t, terms = chains(
        eigen_basis, eigen_rates, guess_coarse[0], initial_state, force_fine[0], force_coarse[0]
    )
    fine_next = shift(force_fine[0], -1)
    states = coarse_solve(terms, carried, coarse_decay)
    coarse_new, fine_new = stages(
        "IEI", (0, 2), 3, basis=(basis, basis_t), decay=fine_decay, start=states, sources=[fine_next], fixed=initial_state
    )
    return (shift(fine_new, 1)[None], coarse_new[None])


def solution(mesh):
    placed = (
        P("space", None),
        P("tm", "space", None),
        P("tm", "space", None),
        P("tm", "space", None),
        P(),
        P(),
        P(),
    )
    return jax.shard_map(
        on_device,
        mesh=mesh,
        in_specs=placed,
        out_specs=(P("tm", "space", None), P("tm", "space", None)),
        check_vma=False,
    )
```

```python
import functools
import jax
import jax.numpy as jnp
from jax import lax
from jax.experimental import pallas as pl
from jax.experimental.pallas import tpu as pltpu
from jax.sharding import PartitionSpec as P

MESH = pl.DeviceIdType.MESH


def halves(block):
    high = block.astype(jnp.bfloat16)
    return high, (block - high.astype(jnp.float32)).astype(jnp.bfloat16)


def dot3(left, right):
    dot = functools.partial(jnp.dot, preferred_element_type=jnp.float32)
    return dot(left[0], right[0]) + dot(left[0], right[1]) + dot(left[1], right[0])


def reacted(value):
    return value + 0.5 * jnp.tanh(value)


def chain_kernel(
    raw, rates_tall, rates_wide, guess, initial, fine, coarse, basis, basis_t, terms, fine_next,
    before, entry, coarse_next, slots, field, coeffs, kept, wide, tall, part, sent, held, decay, coarse_decay, leaving, landed,
    home_send, shift_send, shift_recv, slot_recv, ex_send, ex_recv, term_send, term_recv,
):
    groups, count = lax.axis_size("tm"), lax.axis_size("space")
    t, s = lax.axis_index("tm"), lax.axis_index("space")
    grid = raw.shape[0]
    rows = fine.shape[0]
    short = rows // 2
    half = grid // 2
    piece = half // 2
    per_half = count // 2
    low_seat = per_half - 1
    last = groups - 1

    def at(start, size):
        return pl.ds(pl.multiple_of(start, size), size)

    def seat(chain):
        return low_seat + chain % 2

    def core(chain, which):
        return 2 * (chain // 2) + which

    position = s % per_half
    group_at = (core(t, s // per_half), seat(t))
    to_self = (group_at[0] == t) & (group_at[1] == s)
    following, preceding = (t + 1) % groups, (t + groups - 1) % groups

    def remote(src, dst, send, recv, where):
        return pltpu.make_async_remote_copy(
            src_ref=src, dst_ref=dst, send_sem=send, recv_sem=recv,
            device_id={"tm": where[0], "space": where[1]}, device_id_type=MESH,
        )

    def group_copy(src, slot, k):
        part_of = src.at[at(k * short, short)]
        dst = slots.at[slot, at(position * rows + k * short, short)]
        return part_of, dst, home_send.at[slot, k], slot_recv.at[slot, 2 * position + k]

    def to_group(src, slot, k):
        part_of, dst, send, recv = group_copy(src, slot, k)

        @pl.when(jnp.logical_not(to_self))
        def _():
            remote(part_of, dst, send, recv, group_at).start()

        @pl.when(to_self)
        def _():
            pltpu.make_async_copy(part_of, dst, recv).start()

    def pass_on(index, src, dst, where):
        return remote(src, dst, shift_send.at[index], shift_recv.at[index], (where, s))

    pass_guess = pass_on(0, guess, before, following)
    pass_fine = pass_on(1, fine, fine_next, preceding)
    pass_entry = pass_on(1, entry, fine_next, preceding)
    pass_coarse = pass_on(2, coarse, coarse_next, preceding)

    @pl.when(t != last)
    def _():
        pass_guess.start()

    @pl.when(t != 0)
    def _():
        pass_fine.start()

    @pl.when(t == 0)
    def _():
        entry[...] = reacted(initial[...]) + fine[...]
        pass_entry.start()

    pass_coarse.start()

    @pl.when(t % 2 == 0)
    def _():
        to_group(coarse, 1, 0)

    @pl.when(t != 0)
    def _():
        pass_guess.wait_recv()
        entry[...] = reacted(before[...]) + fine[...]

    to_group(entry, 0, 0)
    to_group(entry, 0, 1)

    @pl.when(t % 2 == 1)
    def _():
        to_group(coarse, 1, 0)

    to_group(coarse, 1, 1)

    @pl.loop(0, count)
    def _(r):
        high, low = halves(raw[at(r * rows, rows), :])
        basis[0, at(r * rows, rows), :] = high
        basis[1, at(r * rows, rows), :] = low

    pass_fine.wait_recv()
    to_group(fine_next, 2, 0)
    to_group(fine_next, 2, 1)
    pass_coarse.wait_recv()
    to_group(coarse_next, 3, 0)
    to_group(coarse_next, 3, 1)

    @pl.loop(0, grid // piece)
    def _(r):
        @pl.loop(0, grid // piece)
        def _(c):
            high, low = halves(raw[at(c * piece, piece), at(r * piece, piece)].T)
            basis_t[0, at(r * piece, piece), at(c * piece, piece)] = high
            basis_t[1, at(r * piece, piece), at(c * piece, piece)] = low

    side = t % 2
    group = 2 * (t // 2) + (s - low_seat)
    partner = (core(t, 1 - side), s)
    own, other = at(side * half, half), at((1 - side) * half, half)

    def wait_slot(slot, index):
        local = (group == t) & (side * per_half + index == s)
        for k in range(2):
            dst = slots.at[slot, at(index * rows + k * short, short)]
            src, recv = fine.at[at(k * short, short)], slot_recv.at[slot, 2 * index + k]

            @pl.when(jnp.logical_not(local))
            def _():
                remote(src, dst, home_send.at[slot, k], recv, (t, s)).wait_recv()

            @pl.when(local)
            def _():
                pltpu.make_async_copy(src, dst, recv).wait()

    def exchange(stage, m):
        block = at(m * piece, piece)
        return remote(sent.at[stage % 2, block], held.at[stage % 2, block], ex_send.at[stage, m], ex_recv.at[stage, m], partner)

    def collect(stage):
        for m in range(2):
            exchange(stage, m).wait_recv()
            part[0, m * piece:(m + 1) * piece, :], part[1, m * piece:(m + 1) * piece, :] = halves(
                held[stage % 2, m * piece:(m + 1) * piece, :]
            )

    def take(stage, make):
        if stage >= 2:
            for m in range(2):
                exchange(stage - 2, m).wait_send()

        @pl.loop(0, 2)
        def _(m):
            sent[stage % 2, at(m * piece, piece)] = make(m, False)
            exchange(stage, m).start()

        @pl.loop(0, 2)
        def _(m):
            block = at(m * piece, piece)
            part[0, block, :], part[1, block, :] = halves(make(m, True))

    def forward(stage, source, ready, finish):
        for m in range(per_half):
            ready(m)
            high, low = halves(source(at(m * rows, rows)))
            wide[0, at(m * rows, rows), :] = high
            wide[1, at(m * rows, rows), :] = low

        def make(m, keep):
            block, columns = at(m * piece, piece), own if keep else other
            return dot3((wide[0, block, :], wide[1, block, :]), (basis[0, :, columns], basis[1, :, columns]))

        take(stage, make)

        @pl.loop(0, grid // piece)
        def _(r):
            block = at(r * piece, piece)
            coeffs[block, :] = dot3((basis_t[0, block, own], basis_t[1, block, own]), (part[0], part[1]))

        collect(stage)

        @pl.loop(0, grid // piece)
        def _(r):
            block = at(r * piece, piece)
            term = dot3((basis_t[0, block, other], basis_t[1, block, other]), (part[0], part[1]))
            finish(r, block, (coeffs[block, :] + term) * decay[block, :])

    def inverse(stage):
        @pl.loop(0, grid // piece)
        def _(r):
            block = at(r * piece, piece)
            tall[0, block, :], tall[1, block, :] = halves(coeffs[block, :])

        def make(m, keep):
            block = at((side if keep else 1 - side) * half + m * piece, piece)
            return dot3((basis[0, block, :], basis[1, block, :]), (tall[0], tall[1]))

        take(stage, make)

        @pl.loop(0, 2)
        def _(n):
            columns = at(n * half, half)
            field[:, columns] = dot3((part[0], part[1]), (basis_t[0, own, columns], basis_t[1, own, columns]))

        collect(stage)

        @pl.loop(0, 2)
        def _(n):
            columns = at(n * half, half)
            field[:, columns] = field[:, columns] + dot3(
                (part[0], part[1]), (basis_t[0, other, columns], basis_t[1, other, columns])
            )

    @pl.when((s == low_seat) | (s == low_seat + 1))
    def _():
        @pl.loop(0, grid // piece)
        def _(r):
            block = at(r * piece, piece)
            pair = rates_tall[block, :1] + rates_wide[:1, own]
            decay[block, :] = 1.0 / (1.0 + pair)
            coarse_decay[block, :] = 1.0 / (1.0 + 2.0 * pair)

        def plain(r, block, value):
            coeffs[block, :] = value

        def keep(r, block, value):
            coeffs[block, :] = value
            kept[block, :] = jnp.where(group == last, 0.0, value * coarse_decay[block, :])

        def leave(r, block, value):
            value = value - kept[block, :]
            for q in range(per_half):
                leaving[q, block, :] = value[:, q * rows:(q + 1) * rows]
            for q in range(per_half):
                send_term(r, q)

        def term_place(q):
            return group, side * per_half + q

        def term_copy(r, q):
            block = at(r * piece, piece)
            return remote(leaving.at[q, block], landed.at[block], term_send.at[q, r], term_recv.at[r], term_place(q))

        def term_local(r, q):
            block = at(r * piece, piece)
            return pltpu.make_async_copy(leaving.at[q, block], landed.at[block], term_recv.at[r])

        def term_here(q):
            where = term_place(q)
            return (where[0] == t) & (where[1] == s)

        def send_term(r, q):
            here = term_here(q)

            @pl.when(here)
            def _():
                term_local(r, q).start()

            @pl.when(jnp.logical_not(here))
            def _():
                term_copy(r, q).start()

        def from_field(slot):
            def source(block):
                moved = reacted(field[block, :])
                if slot == 2:
                    moved = jnp.where(group == last, 0.0, moved)
                return moved + slots[slot, block, :]
            return source

        forward(0, lambda block: slots[0, block, :], lambda m: wait_slot(0, m), plain)
        inverse(1)
        forward(2, from_field(1), lambda m: wait_slot(1, m), keep)
        inverse(3)
        forward(4, from_field(2), lambda m: wait_slot(2, m), plain)
        inverse(5)
        forward(6, from_field(3), lambda m: wait_slot(3, m), leave)

        for stage in (5, 6):
            for m in range(2):
                exchange(stage, m).wait_send()
        for q in range(per_half):
            @pl.when(jnp.logical_not(term_here(q)))
            def _():
                for r in range(grid // piece):
                    term_copy(r, q).wait_send()

    term_side = s // per_half
    sender = (core(t, term_side), seat(t))
    from_self = (sender[0] == t) & (sender[1] == s)
    for r in range(grid // piece):
        block = at(r * piece, piece)

        @pl.when(from_self)
        def _():
            pltpu.make_async_copy(leaving.at[0, block], landed.at[block], term_recv.at[r]).wait()

        @pl.when(jnp.logical_not(from_self))
        def _():
            remote(leaving.at[0, block], landed.at[block], term_send.at[0, r], term_recv.at[r], (t, s)).wait_recv()

        terms[block, :] = landed[block, :]

    @pl.when(jnp.logical_not(to_self))
    def _():
        for slot, src in enumerate((entry, coarse, fine_next, coarse_next)):
            for k in range(2):
                remote(*group_copy(src, slot, k), group_at).wait_send()

    @pl.when(t != last)
    def _():
        pass_guess.wait_send()

    pass_fine.wait_send()
    pass_coarse.wait_send()


def chains(basis, rates, guess, initial, fine, coarse):
    grid, rows = basis.shape[0], fine.shape[0]
    half = grid // 2
    piece, count = half // 2, grid // rows
    per_half = count // 2
    steps = 7
    f32, bf16 = jnp.float32, jnp.bfloat16
    lanes = 128
    operands = [basis, jnp.broadcast_to(rates[:, None], (grid, lanes)), rates[None, :], guess, initial, fine, coarse]
    shapes = [
        jax.ShapeDtypeStruct((2, grid, grid), bf16),
        jax.ShapeDtypeStruct((2, grid, grid), bf16),
        jax.ShapeDtypeStruct((grid, rows), f32),
        jax.ShapeDtypeStruct((rows, grid), f32),
    ]
    vmem = pl.BlockSpec(memory_space=pltpu.VMEM)
    dma = pltpu.SemaphoreType.DMA
    return pl.pallas_call(
        chain_kernel,
        out_shape=shapes,
        in_specs=[vmem] * len(operands),
        out_specs=[vmem] * len(shapes),
        scratch_shapes=[
            pltpu.VMEM((rows, grid), f32),
            pltpu.VMEM((rows, grid), f32),
            pltpu.VMEM((rows, grid), f32),
            pltpu.VMEM((4, half, grid), f32),
            pltpu.VMEM((half, grid), f32),
            pltpu.VMEM((grid, half), f32),
            pltpu.VMEM((grid, half), f32),
            pltpu.VMEM((2, half, grid), bf16),
            pltpu.VMEM((2, grid, half), bf16),
            pltpu.VMEM((2, half, half), bf16),
            pltpu.VMEM((2, half, half), f32),
            pltpu.VMEM((2, half, half), f32),
            pltpu.VMEM((grid, half), f32),
            pltpu.VMEM((grid, half), f32),
            pltpu.VMEM((per_half, grid, rows), f32),
            pltpu.VMEM((grid, rows), f32),
            dma((4, 2)),
            dma((3,)),
            dma((3,)),
            dma((4, count)),
            dma((steps, 2)),
            dma((steps, 2)),
            dma((per_half, grid // piece)),
            dma((grid // piece,)),
        ],
        compiler_params=pltpu.CompilerParams(has_side_effects=True, vmem_limit_bytes=62 * 1024 * 1024),
        cost_estimate=pl.CostEstimate(flops=150_000_000_000, bytes_accessed=16 * grid * grid, transcendentals=0),
        name="chains",
    )(*operands)


def stages_kernel(
    plan, forced, raw, basis, basis_t, spare, decay, start, sources, fixed, outs, split, split_tall, field, coeffs, sent, held, doubled, send_sem, recv_sem
):
    count = lax.axis_size("space")
    me = lax.axis_index("space")
    rows = held.shape[2]
    barrier = pltpu.get_barrier_semaphore()

    @pl.loop(0, count)
    def _(d):
        @pl.when(d != me)
        def _():
            pl.semaphore_signal(barrier, inc=1, device_id={"space": d}, device_id_type=pl.DeviceIdType.MESH)

    pl.semaphore_wait(barrier, count - 1)

    def span(d):
        return pl.ds(pl.multiple_of(d * rows, rows), rows)

    def peer(k):
        return jnp.where(me < count // 2, count - 1 - k, k)

    def copy(stage, d):
        return pltpu.make_async_remote_copy(
            src_ref=sent.at[stage, d],
            dst_ref=held.at[stage, me],
            send_sem=send_sem.at[stage, d],
            recv_sem=recv_sem.at[stage, me],
            device_id={"space": d},
            device_id_type=pl.DeviceIdType.MESH,
        )

    def arrival(stage, s):
        return pltpu.make_async_remote_copy(
            src_ref=sent.at[stage, s],
            dst_ref=held.at[stage, s],
            send_sem=send_sem.at[stage, s],
            recv_sem=recv_sem.at[stage, s],
            device_id={"space": s},
            device_id_type=pl.DeviceIdType.MESH,
        )

    def exchange(stage, block_for, use, between=None):
        @pl.loop(0, count)
        def _(k):
            d = peer(k)
            block = block_for(d)

            @pl.when(d != me)
            def _():
                sent[stage, d] = block
                copy(stage, d).start()

            @pl.when(d == me)
            def _():
                held[stage, me] = block

        if between is not None:
            between()
        use(me, True)

        @pl.loop(0, count)
        def _(k):
            s = peer(k)

            @pl.when(s != me)
            def _():
                arrival(stage, s).wait_recv()
                use(s, False)

    def split_basis():
        @pl.loop(0, count)
        def _(r):
            high, low = halves(raw[span(r), :])
            basis[0, span(r), :] = high
            basis[1, span(r), :] = low

    def turn_basis():
        @pl.loop(0, count)
        def _(r):
            @pl.loop(0, count)
            def _(c):
                high, low = halves(raw[span(c), span(r)].T)
                basis_t[0, span(r), span(c)] = high
                basis_t[1, span(r), span(c)] = low

    def forward(stage):
        high, low = halves(field[...])
        split[0] = high
        split[1] = low

        def block_for(d):
            return dot3((split[0], split[1]), (basis[0, :, span(d)], basis[1, :, span(d)]))

        def use(s, first):
            part = halves(held[stage, s])

            @pl.loop(0, count)
            def _(r):
                term = dot3((basis_t[0, span(r), span(s)], basis_t[1, span(r), span(s)]), part)
                coeffs[span(r), :] = term if first else coeffs[span(r), :] + term

        exchange(stage, block_for, use, turn_basis if raw is not None and stage == 0 else None)

    def inverse(stage):
        high, low = halves(coeffs[...])
        split_tall[0] = high
        split_tall[1] = low

        def block_for(d):
            block = dot3((basis[0, span(d), :], basis[1, span(d), :]), (split_tall[0], split_tall[1]))
            if spare is not None and stage == len(plan) - 1:
                doubled[0, span(d), :], doubled[1, span(d), :] = halves(block)
            return block

        def keep_spare():
            @pl.loop(0, count)
            def _(r):
                back = dot3((basis_t[0, span(r), :], basis_t[1, span(r), :]), (doubled[0], doubled[1]))
                spare[span(r), :] = back - coeffs[span(r), :]

        def use(s, first):
            part = halves(held[stage, s])

            @pl.loop(0, count)
            def _(r):
                term = dot3(part, (basis_t[0, span(s), span(r)], basis_t[1, span(s), span(r)]))
                field[:, span(r)] = term if first else field[:, span(r)] + term

        exchange(stage, block_for, use, keep_spare if spare is not None and stage == len(plan) - 1 else None)

    def react(source):
        value = field[...]
        moved = jnp.where(lax.axis_index("tm") == lax.axis_size("tm") - 1, 0.0, value + 0.5 * jnp.tanh(value))
        field[...] = moved + source[...]

    sources = list(sources)
    outs = list(outs)
    if raw is not None:
        split_basis()
    if plan[0] == "E":
        field[...] = start[...]
        react(sources.pop(0))
    else:
        coeffs[...] = start[...]
    for stage, kind in enumerate(plan):
        final = stage == len(plan) - 1
        if kind == "E":
            forward(stage)
            coeffs[...] = coeffs[...] * decay[...]
            if stage in forced:
                outs.pop(0)[...] = coeffs[...]
        else:
            inverse(stage)
            if stage in forced:
                outs.pop(0)[...] = field[...]
            if not final:
                react(sources.pop(0))

    for stage in range(len(plan)):
        @pl.loop(0, count)
        def _(d):
            @pl.when(d != me)
            def _():
                copy(stage, d).wait_send()


def stages(plan, forced, number, basis, decay, start, sources, fixed=None):
    grid, rows = decay.shape
    count = grid // rows
    wide, tall = (rows, grid), (grid, rows)
    extra = 0 if fixed is None else 1
    first = not isinstance(basis, tuple)
    given = [basis] if first else list(basis)
    shapes = [jax.ShapeDtypeStruct(tall if plan[s] == "E" else wide, jnp.float32) for s in forced]
    if first:
        shapes += [jax.ShapeDtypeStruct((2, grid, grid), jnp.bfloat16)] * 2 + [jax.ShapeDtypeStruct(tall, jnp.float32)]

    def kernel(*refs):
        refs = list(refs)
        basis_refs = refs[: len(given)]
        del refs[: len(given)]
        decay_ref, start_ref = refs[:2]
        del refs[:2]
        source_refs = refs[: len(sources)]
        del refs[: len(sources)]
        fixed_ref = refs.pop(0) if extra else None
        out_refs = refs[: len(shapes)]
        raw, spare = None, None
        if first:
            raw = basis_refs[0]
            basis_refs, spare = out_refs[-3:-1], out_refs[-1]
        stages_kernel(
            plan, forced, raw, *basis_refs, spare, decay_ref, start_ref, source_refs, fixed_ref, out_refs, *refs[len(shapes):]
        )

    operands = [*given, decay, start, *sources] + ([fixed] if extra else [])
    steps = len(plan)
    vmem = pl.BlockSpec(memory_space=pltpu.VMEM)
    return pl.pallas_call(
        kernel,
        out_shape=shapes,
        in_specs=[vmem] * len(operands),
        out_specs=[vmem] * len(shapes),
        scratch_shapes=[
            pltpu.VMEM((2, *wide), jnp.bfloat16),
            pltpu.VMEM((2, *tall), jnp.bfloat16),
            pltpu.VMEM(wide, jnp.float32),
            pltpu.VMEM(tall, jnp.float32),
            pltpu.VMEM((steps, count, rows, rows), jnp.float32),
            pltpu.VMEM((steps, count, rows, rows), jnp.float32),
            pltpu.VMEM((2, *tall) if first else (2, 16, 128), jnp.bfloat16),
            pltpu.SemaphoreType.DMA((steps, count)),
            pltpu.SemaphoreType.DMA((steps, count)),
        ],
        compiler_params=pltpu.CompilerParams(
            collective_id=number, has_side_effects=True, vmem_limit_bytes=48 * 1024 * 1024
        ),
        cost_estimate=pl.CostEstimate(
            flops=steps * 40_000_000_000, bytes_accessed=8 * grid * grid, transcendentals=0
        ),
        name="stages_%d" % number,
    )(*operands)


def decay_block(eigen_rates, own_rates, factor):
    return 1.0 / (1.0 + factor * (eigen_rates[:, None] + own_rates[None, :]))


def shift(block, distance):
    count = lax.axis_size("tm")
    return lax.ppermute(block, "tm", [(i, (i + distance) % count) for i in range(count)])


def swap(block):
    count = lax.axis_size("tm")
    return lax.ppermute(block, "tm", [(i, i ^ 1) for i in range(count)])


def coarse_solve(terms, start, decay):
    count = lax.axis_size("tm")
    pairs = count // 2
    place = lax.axis_index("tm")
    pair, odd = place // 2, place % 2
    half = terms.shape[0] // 2

    def mine(block, which):
        return lax.dynamic_slice_in_dim(block, which * half, half, 0)

    other = swap(mine(terms, 1 - odd))
    own = mine(terms, odd)
    first = jnp.where(odd == 0, own, other)
    second = jnp.where(odd == 0, other, own)
    decay = mine(decay, odd)
    carried = mine(start, odd)
    is_last = pair == pairs - 1
    sums = second + decay * jnp.where(is_last, carried, first)
    squared = decay * decay
    before = jnp.where(is_last, sums, 0.0)
    arrived = {}
    for s in range(1, pairs):
        route = []
        for k in range(pairs):
            if s <= k + 1:
                source = (k - s) % pairs
                route += [(2 * source + c, 2 * k + c) for c in range(2)]
        arrived[s] = lax.ppermute(sums, "tm", route)
    for s in range(pairs - 1, 0, -1):
        before = squared * before + arrived[s]
    even_state = before
    odd_state = first + decay * even_state
    given = jnp.where(odd == 0, odd_state, even_state)
    kept = jnp.where(odd == 0, even_state, odd_state)
    got = swap(given)
    return jnp.where(
        odd == 0,
        jnp.concatenate([kept, got], 0),
        jnp.concatenate([got, kept], 0),
    )


def on_device(
    initial_state,
    guess_coarse,
    force_fine,
    force_coarse,
    eigen_basis,
    eigen_rates,
    carried_correction,
):
    row_count = initial_state.shape[0]
    offset = lax.axis_index("space") * row_count
    own_rates = lax.dynamic_slice_in_dim(eigen_rates, offset, row_count, 0)
    fine_decay = decay_block(eigen_rates, own_rates, 1.0)
    coarse_decay = decay_block(eigen_rates, own_rates, 2.0)
    carried = lax.dynamic_slice_in_dim(carried_correction, offset, row_count, 1)
    place = lax.axis_index("tm")
    basis, basis_t, terms, fine_next = chains(
        eigen_basis, eigen_rates, guess_coarse[0], initial_state, force_fine[0], force_coarse[0]
    )
    states = coarse_solve(terms, carried, coarse_decay)
    coarse_new, fine_new = stages(
        "IEI", (0, 2), 3, basis=(basis, basis_t), decay=fine_decay, start=states, sources=[fine_next]
    )
    return (shift(fine_new, 1)[None], coarse_new[None])


def solution(mesh):
    placed = (
        P("space", None),
        P("tm", "space", None),
        P("tm", "space", None),
        P("tm", "space", None),
        P(),
        P(),
        P(),
    )
    return jax.shard_map(
        on_device,
        mesh=mesh,
        in_specs=placed,
        out_specs=(P("tm", "space", None), P("tm", "space", None)),
        check_vma=False,
    )
```

```python
import functools
import jax
import jax.numpy as jnp
from jax import lax
from jax.experimental import pallas as pl
from jax.experimental.pallas import tpu as pltpu
from jax.sharding import PartitionSpec as P

MESH = pl.DeviceIdType.MESH


def halves(block):
    high = block.astype(jnp.bfloat16)
    return high, (block - high.astype(jnp.float32)).astype(jnp.bfloat16)


def dot3(left, right):
    dot = functools.partial(jnp.dot, preferred_element_type=jnp.float32)
    return dot(left[0], right[0]) + dot(left[0], right[1]) + dot(left[1], right[0])


def reacted(value):
    return value + 0.5 * jnp.tanh(value)


def cycle_kernel(
    raw, rates, guess, initial, fine, coarse, carried, fine_out, coarse_out,
    basis, basis_t, rates_tall, before, entry, fine_next, coarse_next, slots, field, coeffs, kept, wide, tall, part,
    sent, held, decay, landed, joined, gathered, evens, got, crossed, start,
    home_send, shift_send, shift_recv, slot_recv, ex_send, ex_recv, term_send, term_recv,
    pair_send, pair_recv, share_send, share_recv, cross_send, cross_recv, start_sem,
):
    groups, count = lax.axis_size("tm"), lax.axis_size("space")
    t, s = lax.axis_index("tm"), lax.axis_index("space")
    grid = raw.shape[0]
    rows = fine.shape[0]
    short = rows // 2
    half = grid // 2
    piece = half // 2
    pieces = grid // piece
    per_half = count // 2
    low_seat = per_half - 1
    last = groups - 1
    lanes = rates_tall.shape[1]
    cuts = rows // lanes
    pairs = groups // 2
    share = half // pairs

    def at(start, size):
        return pl.ds(pl.multiple_of(start, size), size)

    def span(d):
        return at(d * rows, rows)

    def seat(chain):
        return low_seat + chain % 2

    def core(chain, which):
        return 2 * (chain // 2) + which

    def remote(src, dst, send, recv, where):
        return pltpu.make_async_remote_copy(
            src_ref=src, dst_ref=dst, send_sem=send, recv_sem=recv,
            device_id={"tm": where[0], "space": where[1]}, device_id_type=MESH,
        )

    position = s % per_half
    group_at = (core(t, s // per_half), seat(t))
    to_self = (group_at[0] == t) & (group_at[1] == s)
    following, preceding = (t + 1) % groups, (t + groups - 1) % groups

    def group_copy(src, slot, k):
        part_of = src.at[at(k * short, short)]
        dst = slots.at[slot, at(position * rows + k * short, short)]
        return part_of, dst, home_send.at[slot, k], slot_recv.at[slot, 2 * position + k]

    def to_group(src, slot, k):
        part_of, dst, send, recv = group_copy(src, slot, k)

        @pl.when(jnp.logical_not(to_self))
        def _():
            remote(part_of, dst, send, recv, group_at).start()

        @pl.when(to_self)
        def _():
            pltpu.make_async_copy(part_of, dst, recv).start()

    def pass_on(index, src, dst, where):
        return remote(src, dst, shift_send.at[index], shift_recv.at[index], (where, s))

    pass_guess = pass_on(0, guess, before, following)
    pass_fine = pass_on(1, fine, fine_next, preceding)
    pass_entry = pass_on(1, entry, fine_next, preceding)
    pass_coarse = pass_on(2, coarse, coarse_next, preceding)

    side = t % 2
    pair = t // 2
    own, other = at(side * half, half), at((1 - side) * half, half)
    partner = (core(t, 1 - side), s)
    start_copy = pltpu.make_async_copy(
        carried.at[at(side * half + pair * share, share), span(s)], start, start_sem.at[0]
    )

    @pl.when(t != last)
    def _():
        pass_guess.start()

    @pl.when(t != 0)
    def _():
        pass_fine.start()

    @pl.when(t == 0)
    def _():
        entry[...] = reacted(initial[...]) + fine[...]
        pass_entry.start()

    pass_coarse.start()
    start_copy.start()

    @pl.when(t % 2 == 0)
    def _():
        to_group(coarse, 1, 0)

    @pl.when(t != 0)
    def _():
        pass_guess.wait_recv()
        entry[...] = reacted(before[...]) + fine[...]

    to_group(entry, 0, 0)
    to_group(entry, 0, 1)

    @pl.when(t % 2 == 1)
    def _():
        to_group(coarse, 1, 0)

    to_group(coarse, 1, 1)

    @pl.loop(0, count)
    def _(r):
        high, low = halves(raw[span(r), :])
        basis[0, span(r), :] = high
        basis[1, span(r), :] = low

    pass_fine.wait_recv()
    to_group(fine_next, 2, 0)
    to_group(fine_next, 2, 1)
    pass_coarse.wait_recv()
    to_group(coarse_next, 3, 0)
    to_group(coarse_next, 3, 1)

    @pl.loop(0, pieces)
    def _(r):
        @pl.loop(0, pieces)
        def _(c):
            high, low = halves(raw[at(c * piece, piece), at(r * piece, piece)].T)
            basis_t[0, at(r * piece, piece), at(c * piece, piece)] = high
            basis_t[1, at(r * piece, piece), at(c * piece, piece)] = low

    @pl.loop(0, grid // lanes)
    def _(r):
        rates_tall[at(r * lanes, lanes), :] = jnp.broadcast_to(rates[:, at(r * lanes, lanes)], (lanes, lanes)).T

    def sums_of_rates(block, columns):
        return rates_tall[block, :1] + rates[:, columns]

    def fine_decay(block, columns):
        return 1.0 / (1.0 + sums_of_rates(block, columns))

    def coarse_decay(block, columns):
        return 1.0 / (1.0 + 2.0 * sums_of_rates(block, columns))

    group = core(t, s - low_seat)

    def wait_slot(slot, index):
        local = (group == t) & (side * per_half + index == s)
        for k in range(2):
            dst = slots.at[slot, at(index * rows + k * short, short)]
            src, recv = fine.at[at(k * short, short)], slot_recv.at[slot, 2 * index + k]

            @pl.when(jnp.logical_not(local))
            def _():
                remote(src, dst, home_send.at[slot, k], recv, (t, s)).wait_recv()

            @pl.when(local)
            def _():
                pltpu.make_async_copy(src, dst, recv).wait()

    def exchange(stage, m):
        block = at(m * piece, piece)
        return remote(sent.at[stage % 2, block], held.at[stage % 2, block], ex_send.at[stage, m], ex_recv.at[stage, m], partner)

    def halves_to(ref, index, value):
        ref[(0, *index)], ref[(1, *index)] = halves(value)

    def reorder(value, order):
        if not order:
            return value
        return jnp.concatenate(
            [value[:, q * rows + h * lanes:q * rows + (h + 1) * lanes] for h in range(cuts) for q in range(per_half)], 1
        )

    def collect(stage, into, order=False):
        for m in range(2):
            block = at(m * piece, piece)
            exchange(stage, m).wait_recv()
            halves_to(into, (block, slice(0, half)), reorder(held[stage % 2, block, :], order))

    def free(stage):
        if stage >= 2:
            for m in range(2):
                exchange(stage - 2, m).wait_send()

    def right_of(stage, source, slot, order=False):
        free(stage)
        for m in range(2):
            block = at(m * piece, piece)
            for index in range(m * per_half // 2, (m + 1) * per_half // 2):
                wait_slot(slot, index)
            halves_to(wide, (block, slice(None)), source(block))
            left = (wide[0, block, :], wide[1, block, :])
            sent[stage % 2, block] = dot3(left, (basis[0, :, other], basis[1, :, other]))
            exchange(stage, m).start()
            halves_to(part, (block, slice(None)), reorder(dot3(left, (basis[0, :, own], basis[1, :, own])), order))

    def forward(stage, source, slot, finish):
        right_of(stage, source, slot)

        @pl.loop(0, 2)
        def _(n):
            columns = at(n * piece, piece)
            coeffs[:, columns] = dot3((basis_t[0, :, own], basis_t[1, :, own]), (part[0, :, columns], part[1, :, columns]))

        collect(stage, part)

        @pl.loop(0, 2)
        def _(n):
            columns = at(n * piece, piece)
            term = dot3((basis_t[0, :, other], basis_t[1, :, other]), (part[0, :, columns], part[1, :, columns]))
            value = (coeffs[:, columns] + term) * decay[:, columns]
            coeffs[:, columns] = value
            finish(n, columns, value)

    def inverse(stage):
        free(stage)

        @pl.loop(0, pieces)
        def _(r):
            block = at(r * piece, piece)
            halves_to(tall, (block, slice(None)), coeffs[block, :])

        def rows_of(m, which):
            block = at(which * half + m * piece, piece)
            return dot3((basis[0, block, :], basis[1, block, :]), (tall[0], tall[1]))

        @pl.loop(0, 2)
        def _(m):
            sent[stage % 2, at(m * piece, piece)] = rows_of(m, 1 - side)
            exchange(stage, m).start()

        @pl.loop(0, 2)
        def _(m):
            halves_to(part, (at(m * piece, piece), slice(None)), rows_of(m, side))

        @pl.loop(0, 2)
        def _(n):
            columns = at(n * half, half)
            field[:, columns] = dot3((part[0], part[1]), (basis_t[0, own, columns], basis_t[1, own, columns]))

        collect(stage, part)

        @pl.loop(0, 2)
        def _(n):
            columns = at(n * half, half)
            field[:, columns] = field[:, columns] + dot3(
                (part[0], part[1]), (basis_t[0, other, columns], basis_t[1, other, columns])
            )

    def term_place(q):
        return group, side * per_half + q

    def term_refs(h, r, q):
        block = at(r * piece, piece)
        source = coeffs.at[block, at((h * per_half + q) * lanes, lanes)]
        return source, landed.at[block, at(h * lanes, lanes)]

    def term_here(q):
        where = term_place(q)
        return (where[0] == t) & (where[1] == s)

    def send_term(h, r, q):
        source, target = term_refs(h, r, q)

        @pl.when(term_here(q))
        def _():
            pltpu.make_async_copy(source, target, term_recv.at[h, r]).start()

        @pl.when(jnp.logical_not(term_here(q)))
        def _():
            remote(source, target, term_send.at[h, r, q], term_recv.at[h, r], term_place(q)).start()

    @pl.when((s == low_seat) | (s == low_seat + 1))
    def _():
        @pl.loop(0, pieces)
        def _(r):
            block = at(r * piece, piece)
            decay[block, :] = fine_decay(block, own)

        def plain(n, columns, value):
            pass

        def keep(n, columns, value):
            taken = value * coarse_decay(slice(None), at(side * half + n * piece, piece))
            kept[:, columns] = jnp.where(group == last, 0.0, taken)

        def from_field(slot):
            def source(block):
                moved = reacted(field[block, :])
                if slot == 2:
                    moved = jnp.where(group == last, 0.0, moved)
                return moved + slots[slot, block, :]
            return source

        forward(0, lambda block: slots[0, block, :], 0, plain)
        inverse(1)
        forward(2, from_field(1), 1, keep)
        inverse(3)
        forward(4, from_field(2), 2, plain)
        inverse(5)

        right_of(6, from_field(3), 3, True)
        collect(6, wide, True)
        for h in range(cuts):
            columns = slice(h * per_half * lanes, (h + 1) * per_half * lanes)

            @pl.loop(0, pieces)
            def _(r):
                block = at(r * piece, piece)
                value = dot3((basis_t[0, block, own], basis_t[1, block, own]), (part[0, :, columns], part[1, :, columns]))
                value = value + dot3(
                    (basis_t[0, block, other], basis_t[1, block, other]), (wide[0, :, columns], wide[1, :, columns])
                )
                for q in range(per_half):
                    natural = slice(q * rows + h * lanes, q * rows + (h + 1) * lanes)
                    coeffs[block, at((h * per_half + q) * lanes, lanes)] = (
                        value[:, q * lanes:(q + 1) * lanes] * decay[block, natural] - kept[block, natural]
                    )
                for q in range(per_half):
                    send_term(h, r, q)

        for stage in (5, 6):
            for m in range(2):
                exchange(stage, m).wait_send()

    sender = (core(t, s // per_half), seat(t))
    from_self = (sender[0] == t) & (sender[1] == s)

    def wait_term(h, r):
        source, target = term_refs(h, r, 0)

        @pl.when(from_self)
        def _():
            pltpu.make_async_copy(source, target, term_recv.at[h, r]).wait()

        @pl.when(jnp.logical_not(from_self))
        def _():
            remote(source, target, term_send.at[h, r, 0], term_recv.at[h, r], (t, s)).wait_recv()

    spread, fanned, given = (slots.at[0, :, at(k * rows, rows)] for k in range(3))

    def cut(h):
        return at(h * lanes, lanes)

    def column_of(h):
        return at(s * rows + h * lanes, lanes)

    def swap_terms(h):
        return remote(landed.at[other, cut(h)], joined.at[:, cut(h)], pair_send.at[0, h], pair_recv.at[0, h], partner)

    def swap_states(h):
        return remote(given.at[:, cut(h)], got.at[:, cut(h)], pair_send.at[1, h], pair_recv.at[1, h], partner)

    def share_out(h, k):
        return remote(
            spread.at[at(k * share, share), cut(h)], gathered.at[pair, :, cut(h)],
            share_send.at[0, h, k], share_recv.at[0, h, pair], (core(2 * k, side), s),
        )

    def share_in(h, k):
        return remote(
            spread.at[at(k * share, share), cut(h)], gathered.at[k, :, cut(h)],
            share_send.at[0, h, k], share_recv.at[0, h, k], (core(2 * k, side), s),
        )

    def fan_out(h, k):
        return remote(
            fanned.at[at(k * share, share), cut(h)], evens.at[at(pair * share, share), cut(h)],
            share_send.at[1, h, k], share_recv.at[1, h, pair], (core(2 * k, side), s),
        )

    def fan_in(h, k):
        return remote(
            fanned.at[at(k * share, share), cut(h)], evens.at[at(k * share, share), cut(h)],
            share_send.at[1, h, k], share_recv.at[1, h, k], (core(2 * k, side), s),
        )

    def elsewhere(act):
        @pl.loop(0, pairs)
        def _(k):
            @pl.when(k != pair)
            def _():
                act(k)

    def solve(h):
        for r in range(pieces):
            wait_term(h, r)
        swap_terms(h).start()
        rate = coarse_decay(own, column_of(h))
        swap_terms(h).wait_recv()
        mine, theirs = landed[own, cut(h)], joined[:, cut(h)]
        first = jnp.where(side == 0, mine, theirs)
        second = jnp.where(side == 0, theirs, mine)
        spread[:, cut(h)] = second + jnp.where(pair == pairs - 1, 0.0, rate * first)
        elsewhere(lambda k: share_out(h, k).start())
        gathered[pair, :, cut(h)] = spread[at(pair * share, share), cut(h)]
        if h == 0:
            start_copy.wait()
        elsewhere(lambda k: share_in(h, k).wait_recv())
        near = coarse_decay(at(side * half + pair * share, share), column_of(h))
        value = gathered[pairs - 1, :, cut(h)] + near * start[:, cut(h)]
        fanned[0:share, cut(h)] = value
        near = near * near
        for k in range(pairs - 1):
            value = gathered[k, :, cut(h)] + near * value
            fanned[(k + 1) * share:(k + 2) * share, cut(h)] = value
        elsewhere(lambda k: fan_out(h, k).start())
        evens[at(pair * share, share), cut(h)] = fanned[at(pair * share, share), cut(h)]
        elsewhere(lambda k: fan_in(h, k).wait_recv())
        even = evens[:, cut(h)]
        odd = first + rate * even
        given[:, cut(h)] = jnp.where(side == 0, odd, even)
        swap_states(h).start()
        halves_to(tall, (own, cut(h)), jnp.where(side == 0, even, odd))
        swap_states(h).wait_recv()
        halves_to(tall, (other, cut(h)), got[:, cut(h)])

    def peer(k):
        return jnp.where(s < count // 2, count - 1 - k, k)

    def cross(stage, d, h, width, to, by):
        window = pl.ds(pl.multiple_of(d * rows + h * width, width), width)
        return remote(
            slots.at[stage + 1, 0:rows, window], crossed.at[stage, by, :, at(h * width, width)],
            cross_send.at[stage, d, h], cross_recv.at[stage, by, h], (to, d),
        )

    def dispatch(stage, h, width, block_for, to, keeps):
        @pl.loop(0, count)
        def _(k):
            d = peer(k)
            block = block_for(d)

            def away():
                slots[stage + 1, 0:rows, pl.ds(pl.multiple_of(d * rows + h * width, width), width)] = block
                cross(stage, d, h, width, to, s).start()

            if keeps:
                pl.when(d != s)(away)

                @pl.when(d == s)
                def _():
                    crossed[stage, s, :, at(h * width, width)] = block
            else:
                away()

    def absorb(stage, parts, width, use, keeps):
        if keeps:
            use(s, True)

        @pl.loop(0, count)
        def _(k):
            d = peer(k)

            def arrive(first):
                for h in range(parts):
                    cross(stage, d, h, width, t, d).wait_recv()
                use(d, first)

            if keeps:
                pl.when(d != s)(lambda: arrive(False))
            else:
                pl.when(k == 0)(lambda: arrive(True))
                pl.when(k != 0)(lambda: arrive(False))

    def left_rows(d, columns):
        return dot3((basis[0, span(d), :], basis[1, span(d), :]), (tall[0, :, columns], tall[1, :, columns]))

    def rows_into(ref, stage):
        def use(d, first):
            block = halves(crossed[stage, d])

            @pl.loop(0, 2)
            def _(n):
                columns = at(n * half, half)
                term = dot3(block, (basis_t[0, span(d), columns], basis_t[1, span(d), columns]))
                ref[:, columns] = term if first else ref[:, columns] + term
        return use

    for h in range(cuts):
        solve(h)
        dispatch(0, h, lanes, lambda d: left_rows(d, slice(h * lanes, (h + 1) * lanes)), t, True)

    absorb(0, cuts, lanes, rows_into(coarse_out, 0), True)
    moved = jnp.where(t == last, 0.0, reacted(coarse_out[...]))
    halves_to(wide, (slice(0, rows), slice(None)), moved + fine_next[...])

    dispatch(
        1, 0, rows,
        lambda d: dot3((wide[0, 0:rows, :], wide[1, 0:rows, :]), (basis[0, :, span(d)], basis[1, :, span(d)])), t, True,
    )

    def columns_use(d, first):
        block = halves(crossed[1, d])

        @pl.loop(0, 2)
        def _(r):
            lines = at(r * half, half)
            term = dot3((basis_t[0, lines, span(d)], basis_t[1, lines, span(d)]), block)
            kept[lines, 0:rows] = term if first else kept[lines, 0:rows] + term

    absorb(1, 1, rows, columns_use, True)

    @pl.loop(0, pieces)
    def _(r):
        block = at(r * piece, piece)
        halves_to(tall, (block, slice(0, rows)), kept[block, 0:rows] * fine_decay(block, span(s)))

    dispatch(2, 0, rows, lambda d: left_rows(d, slice(0, rows)), following, False)
    absorb(2, 1, rows, rows_into(fine_out, 2), False)

    @pl.when((s == low_seat) | (s == low_seat + 1))
    def _():
        for q in range(per_half):
            @pl.when(jnp.logical_not(term_here(q)))
            def _():
                for h in range(cuts):
                    for r in range(pieces):
                        source, target = term_refs(h, r, q)
                        remote(source, target, term_send.at[h, r, q], term_recv.at[h, r], term_place(q)).wait_send()

    @pl.when(jnp.logical_not(to_self))
    def _():
        for slot, source in enumerate((entry, coarse, fine_next, coarse_next)):
            for k in range(2):
                remote(*group_copy(source, slot, k), group_at).wait_send()

    @pl.when(t != last)
    def _():
        pass_guess.wait_send()

    pass_fine.wait_send()
    pass_coarse.wait_send()
    for h in range(cuts):
        swap_terms(h).wait_send()
        swap_states(h).wait_send()
        elsewhere(lambda k: share_out(h, k).wait_send())
        elsewhere(lambda k: fan_out(h, k).wait_send())
    for stage, parts, width, to in ((0, cuts, lanes, t), (1, 1, rows, t), (2, 1, rows, following)):
        @pl.loop(0, count)
        def _(d):
            def leave():
                for h in range(parts):
                    cross(stage, d, h, width, to, s).wait_send()

            if stage == 2:
                leave()
            else:
                pl.when(d != s)(leave)


def on_device(initial, guess, fine, coarse, basis, rates, carried):
    grid, rows = basis.shape[0], initial.shape[0]
    half = grid // 2
    piece, count = half // 2, grid // rows
    per_half, pieces = count // 2, grid // piece
    steps, lanes = 7, 128
    cuts = rows // lanes
    pairs = lax.axis_size("tm") // 2
    share = half // pairs
    f32, bf16 = jnp.float32, jnp.bfloat16
    vmem = pl.BlockSpec(memory_space=pltpu.VMEM)
    dma = pltpu.SemaphoreType.DMA
    fine_new, coarse_new = pl.pallas_call(
        cycle_kernel,
        out_shape=[jax.ShapeDtypeStruct((rows, grid), f32)] * 2,
        in_specs=[vmem] * 6 + [pl.BlockSpec(memory_space=pl.ANY)],
        out_specs=[vmem] * 2,
        scratch_shapes=[
            pltpu.VMEM((2, grid, grid), bf16),
            pltpu.VMEM((2, grid, grid), bf16),
            pltpu.VMEM((grid, lanes), f32),
            pltpu.VMEM((rows, grid), f32),
            pltpu.VMEM((rows, grid), f32),
            pltpu.VMEM((rows, grid), f32),
            pltpu.VMEM((rows, grid), f32),
            pltpu.VMEM((4, half, grid), f32),
            pltpu.VMEM((half, grid), f32),
            pltpu.VMEM((grid, half), f32),
            pltpu.VMEM((grid, half), f32),
            pltpu.VMEM((2, half, grid), bf16),
            pltpu.VMEM((2, grid, half), bf16),
            pltpu.VMEM((2, half, half), bf16),
            pltpu.VMEM((2, half, half), f32),
            pltpu.VMEM((2, half, half), f32),
            pltpu.VMEM((grid, half), f32),
            pltpu.VMEM((grid, rows), f32),
            pltpu.VMEM((half, rows), f32),
            pltpu.VMEM((pairs, share, rows), f32),
            pltpu.VMEM((half, rows), f32),
            pltpu.VMEM((half, rows), f32),
            pltpu.VMEM((3, count, rows, rows), f32),
            pltpu.VMEM((share, rows), f32),
            dma((4, 2)),
            dma((3,)),
            dma((3,)),
            dma((4, count)),
            dma((steps, 2)),
            dma((steps, 2)),
            dma((cuts, pieces, per_half)),
            dma((cuts, pieces)),
            dma((2, cuts)),
            dma((2, cuts)),
            dma((2, cuts, pairs)),
            dma((2, cuts, pairs)),
            dma((3, count, cuts)),
            dma((3, count, cuts)),
            dma((1,)),
        ],
        compiler_params=pltpu.CompilerParams(has_side_effects=True, vmem_limit_bytes=62 * 1024 * 1024),
        cost_estimate=pl.CostEstimate(flops=200_000_000_000, bytes_accessed=16 * grid * grid, transcendentals=0),
        name="cycle",
    )(basis, rates[None, :], guess[0], initial, fine[0], coarse[0], carried)
    return fine_new[None], coarse_new[None]


def solution(mesh):
    placed = (
        P("space", None),
        P("tm", "space", None),
        P("tm", "space", None),
        P("tm", "space", None),
        P(),
        P(),
        P(),
    )
    return jax.shard_map(
        on_device,
        mesh=mesh,
        in_specs=placed,
        out_specs=(P("tm", "space", None), P("tm", "space", None)),
        check_vma=False,
    )
```

```python
import functools
import jax
import jax.numpy as jnp
from jax import lax
from jax.experimental import pallas as pl
from jax.experimental.pallas import tpu as pltpu
from jax.sharding import PartitionSpec as P

MESH = pl.DeviceIdType.MESH


def halves(block):
    high = block.astype(jnp.bfloat16)
    return high, (block - high.astype(jnp.float32)).astype(jnp.bfloat16)


def dot3(left, right):
    dot = functools.partial(jnp.dot, preferred_element_type=jnp.float32)
    return dot(left[0], right[0]) + dot(left[0], right[1]) + dot(left[1], right[0])


def reacted(value):
    return value + 0.5 * jnp.tanh(value)


def cycle_kernel(
    raw, guess, initial, fine, coarse, carried, rates, fine_out, coarse_out,
    basis, basis_t, rates_tall, fine_here, before, entry, fine_next, coarse_next, slots, field, coeffs, kept, wide, tall, part,
    sent, held, decay, landed, joined, gathered, evens, got, crossed, start,
    home_send, shift_send, shift_recv, slot_recv, ex_send, ex_recv, term_send, term_recv,
    pair_send, pair_recv, share_send, share_recv, cross_send, cross_recv, load_sem,
):
    groups, count = lax.axis_size("tm"), lax.axis_size("space")
    t, s = lax.axis_index("tm"), lax.axis_index("space")
    grid = raw.shape[0]
    rows = fine_here.shape[0]
    short = rows // 2
    half = grid // 2
    piece = half // 2
    pieces = grid // piece
    per_half = count // 2
    low_seat = per_half - 1
    last = groups - 1
    lanes = rates_tall.shape[1]
    cuts = rows // lanes
    pairs = groups // 2
    share = half // pairs

    def at(start, size):
        return pl.ds(pl.multiple_of(start, size), size)

    def span(d):
        return at(d * rows, rows)

    def seat(chain):
        return low_seat + chain % 2

    def core(chain, which):
        return 2 * (chain // 2) + which

    def remote(src, dst, send, recv, where):
        return pltpu.make_async_remote_copy(
            src_ref=src, dst_ref=dst, send_sem=send, recv_sem=recv,
            device_id={"tm": where[0], "space": where[1]}, device_id_type=MESH,
        )

    position = s % per_half
    group_at = (core(t, s // per_half), seat(t))
    to_self = (group_at[0] == t) & (group_at[1] == s)
    following, preceding = (t + 1) % groups, (t + groups - 1) % groups

    def group_copy(src, slot, k):
        part_of = src.at[at(k * short, short)]
        dst = slots.at[slot, at(position * rows + k * short, short)]
        return part_of, dst, home_send.at[slot, k], slot_recv.at[slot, 2 * position + k]

    def to_group(src, slot, k):
        part_of, dst, send, recv = group_copy(src, slot, k)

        @pl.when(jnp.logical_not(to_self))
        def _():
            remote(part_of, dst, send, recv, group_at).start()

        @pl.when(to_self)
        def _():
            pltpu.make_async_copy(part_of, dst, recv).start()

    def leave_home(src, slot):
        @pl.when(jnp.logical_not(to_self))
        def _():
            for k in range(2):
                remote(*group_copy(src, slot, k), group_at).wait_send()

    def pass_on(index, src, dst, where):
        return remote(src, dst, shift_send.at[index], shift_recv.at[index], (where, s))

    def pass_guess(k):
        lines = at(k * short, short)
        return pass_on(k, guess.at[lines], before.at[lines], following)

    pass_fine = pass_on(2, fine, fine_next, preceding)
    pass_entry = pass_on(2, entry, fine_next, preceding)
    pass_coarse = pass_on(3, coarse, coarse_next, preceding)

    side = t % 2
    pair = t // 2
    own, other = at(side * half, half), at((1 - side) * half, half)
    partner = (core(t, 1 - side), s)
    start_copy = pltpu.make_async_copy(
        carried.at[at(side * half + pair * share, share), span(s)], start, load_sem.at[0]
    )
    load_fine = pltpu.make_async_copy(fine, fine_here, load_sem.at[1])
    load_initial = pltpu.make_async_copy(initial, before, load_sem.at[2])
    load_low = pltpu.make_async_copy(raw.at[:, 0:half], coeffs, load_sem.at[3])
    load_high = pltpu.make_async_copy(raw.at[:, half:grid], kept, load_sem.at[4])

    @pl.when(t != last)
    def _():
        pass_guess(0).start()
        pass_guess(1).start()

    load_fine.start()

    @pl.when(t == 0)
    def _():
        load_initial.start()

    load_low.start()
    load_high.start()
    start_copy.start()

    @pl.when(t % 2 == 0)
    def _():
        to_group(coarse, 1, 0)

    load_fine.wait()

    @pl.when(t == 0)
    def _():
        load_initial.wait()

    for k in range(2):
        @pl.when(t != 0)
        def _():
            pass_guess(k).wait_recv()

        lines = at(k * short, short)
        entry[lines, :] = reacted(before[lines, :]) + fine_here[lines, :]
        to_group(entry, 0, k)

    @pl.when(t == 0)
    def _():
        pass_entry.start()

    @pl.when(t != 0)
    def _():
        pass_fine.start()

    load_low.wait()
    load_high.wait()
    for which, ref in enumerate((coeffs, kept)):
        @pl.loop(0, count)
        def _(r):
            high, low = halves(ref[span(r), :])
            basis[0, span(r), which * half:(which + 1) * half] = high
            basis[1, span(r), which * half:(which + 1) * half] = low

        @pl.loop(0, pieces)
        def _(c):
            for r in range(2):
                lines = slice(which * half + r * piece, which * half + (r + 1) * piece)
                high, low = halves(ref[at(c * piece, piece), r * piece:(r + 1) * piece].T)
                basis_t[0, lines, at(c * piece, piece)] = high
                basis_t[1, lines, at(c * piece, piece)] = low

    @pl.loop(0, grid // lanes)
    def _(r):
        rates_tall[at(r * lanes, lanes), :] = jnp.broadcast_to(rates[:, at(r * lanes, lanes)], (lanes, lanes)).T

    leave_home(entry, 0)

    @pl.when(t % 2 == 1)
    def _():
        to_group(coarse, 1, 0)

    to_group(coarse, 1, 1)
    pass_coarse.start()

    def home_fine():
        pass_fine.wait_recv()
        to_group(fine_next, 2, 0)
        to_group(fine_next, 2, 1)

    def home_coarse():
        pass_coarse.wait_recv()
        to_group(coarse_next, 3, 0)
        to_group(coarse_next, 3, 1)

    def sums_of_rates(block, columns):
        return rates_tall[block, :1] + rates[:, columns]

    def fine_decay(block, columns):
        return 1.0 / (1.0 + sums_of_rates(block, columns))

    def coarse_decay(block, columns):
        return 1.0 / (1.0 + 2.0 * sums_of_rates(block, columns))

    group = core(t, s - low_seat)

    def wait_slot(slot, index):
        local = (group == t) & (side * per_half + index == s)
        for k in range(2):
            dst = slots.at[slot, at(index * rows + k * short, short)]
            src, recv = entry.at[at(k * short, short)], slot_recv.at[slot, 2 * index + k]

            @pl.when(jnp.logical_not(local))
            def _():
                remote(src, dst, home_send.at[slot, k], recv, (t, s)).wait_recv()

            @pl.when(local)
            def _():
                pltpu.make_async_copy(src, dst, recv).wait()

    def exchange(stage, m):
        block = at(m * piece, piece)
        return remote(sent.at[stage % 2, block], held.at[stage % 2, block], ex_send.at[stage, m], ex_recv.at[stage, m], partner)

    def halves_to(ref, index, value):
        ref[(0, *index)], ref[(1, *index)] = halves(value)

    def reorder(value, order):
        if not order:
            return value
        return jnp.concatenate(
            [value[:, q * rows + h * lanes:q * rows + (h + 1) * lanes] for h in range(cuts) for q in range(per_half)], 1
        )

    def collect(stage, into, order=False):
        for m in range(2):
            block = at(m * piece, piece)
            exchange(stage, m).wait_recv()
            halves_to(into, (block, slice(0, half)), reorder(held[stage % 2, block, :], order))

    def free(stage):
        if stage >= 2:
            for m in range(2):
                exchange(stage - 2, m).wait_send()

    def right_of(stage, source, slot, order=False):
        free(stage)
        for m in range(2):
            block = at(m * piece, piece)
            for index in range(m * per_half // 2, (m + 1) * per_half // 2):
                wait_slot(slot, index)
            halves_to(wide, (block, slice(None)), source(block))
            left = (wide[0, block, :], wide[1, block, :])
            sent[stage % 2, block] = dot3(left, (basis[0, :, other], basis[1, :, other]))
            exchange(stage, m).start()
            halves_to(part, (block, slice(None)), reorder(dot3(left, (basis[0, :, own], basis[1, :, own])), order))

    def forward(stage, source, slot, finish):
        right_of(stage, source, slot)

        @pl.loop(0, 2)
        def _(n):
            columns = at(n * piece, piece)
            coeffs[:, columns] = dot3((basis_t[0, :, own], basis_t[1, :, own]), (part[0, :, columns], part[1, :, columns]))

        collect(stage, part)

        @pl.loop(0, 2)
        def _(n):
            columns = at(n * piece, piece)
            term = dot3((basis_t[0, :, other], basis_t[1, :, other]), (part[0, :, columns], part[1, :, columns]))
            value = (coeffs[:, columns] + term) * decay[:, columns]
            coeffs[:, columns] = value
            finish(n, columns, value)

    def inverse(stage):
        free(stage)

        @pl.loop(0, pieces)
        def _(r):
            block = at(r * piece, piece)
            halves_to(tall, (block, slice(None)), coeffs[block, :])

        def rows_of(m, which):
            block = at(which * half + m * piece, piece)
            return dot3((basis[0, block, :], basis[1, block, :]), (tall[0], tall[1]))

        @pl.loop(0, 2)
        def _(m):
            sent[stage % 2, at(m * piece, piece)] = rows_of(m, 1 - side)
            exchange(stage, m).start()

        @pl.loop(0, 2)
        def _(m):
            halves_to(part, (at(m * piece, piece), slice(None)), rows_of(m, side))

        @pl.loop(0, 2)
        def _(n):
            columns = at(n * half, half)
            field[:, columns] = dot3((part[0], part[1]), (basis_t[0, own, columns], basis_t[1, own, columns]))

        collect(stage, part)

        @pl.loop(0, 2)
        def _(n):
            columns = at(n * half, half)
            field[:, columns] = field[:, columns] + dot3(
                (part[0], part[1]), (basis_t[0, other, columns], basis_t[1, other, columns])
            )

    def term_place(q):
        return group, side * per_half + q

    def term_refs(h, r, q):
        block = at(r * piece, piece)
        source = coeffs.at[block, at((h * per_half + q) * lanes, lanes)]
        return source, landed.at[block, at(h * lanes, lanes)]

    def term_here(q):
        where = term_place(q)
        return (where[0] == t) & (where[1] == s)

    def send_term(h, r, q):
        source, target = term_refs(h, r, q)

        @pl.when(term_here(q))
        def _():
            pltpu.make_async_copy(source, target, term_recv.at[h, r]).start()

        @pl.when(jnp.logical_not(term_here(q)))
        def _():
            remote(source, target, term_send.at[h, r, q], term_recv.at[h, r], term_place(q)).start()

    def leave_terms(h):
        for q in range(per_half):
            @pl.when(jnp.logical_not(term_here(q)))
            def _():
                for r in range(pieces):
                    source, target = term_refs(h, r, q)
                    remote(source, target, term_send.at[h, r, q], term_recv.at[h, r], term_place(q)).wait_send()

    holds = (s == low_seat) | (s == low_seat + 1)

    @pl.when(jnp.logical_not(holds))
    def _():
        leave_home(coarse, 1)
        home_fine()
        leave_home(fine_next, 2)
        home_coarse()

    @pl.when(holds)
    def _():
        @pl.loop(0, pieces)
        def _(r):
            block = at(r * piece, piece)
            decay[block, :] = fine_decay(block, own)

        def plain(n, columns, value):
            pass

        def keep(n, columns, value):
            taken = value * coarse_decay(slice(None), at(side * half + n * piece, piece))
            kept[:, columns] = jnp.where(group == last, 0.0, taken)

        def from_field(slot):
            def source(block):
                moved = reacted(field[block, :])
                if slot == 2:
                    moved = jnp.where(group == last, 0.0, moved)
                return moved + slots[slot, block, :]
            return source

        forward(0, lambda block: slots[0, block, :], 0, plain)
        inverse(1)
        home_fine()
        forward(2, from_field(1), 1, keep)
        inverse(3)
        home_coarse()
        forward(4, from_field(2), 2, plain)
        inverse(5)

        right_of(6, from_field(3), 3, True)
        collect(6, wide, True)
        for h in range(cuts):
            columns = slice(h * per_half * lanes, (h + 1) * per_half * lanes)

            @pl.loop(0, pieces)
            def _(r):
                block = at(r * piece, piece)
                value = dot3((basis_t[0, block, own], basis_t[1, block, own]), (part[0, :, columns], part[1, :, columns]))
                value = value + dot3(
                    (basis_t[0, block, other], basis_t[1, block, other]), (wide[0, :, columns], wide[1, :, columns])
                )
                for q in range(per_half):
                    natural = slice(q * rows + h * lanes, q * rows + (h + 1) * lanes)
                    coeffs[block, at((h * per_half + q) * lanes, lanes)] = (
                        value[:, q * lanes:(q + 1) * lanes] * decay[block, natural] - kept[block, natural]
                    )
                if h == 0:
                    for q in range(per_half):
                        send_term(h, r, q)

            if h > 0:
                leave_terms(h - 1)
                for r in range(pieces):
                    for q in range(per_half):
                        send_term(h, r, q)

        for stage in (5, 6):
            for m in range(2):
                exchange(stage, m).wait_send()

    sender = (core(t, s // per_half), seat(t))
    from_self = (sender[0] == t) & (sender[1] == s)

    def wait_term(h, r):
        source, target = term_refs(h, r, 0)

        @pl.when(from_self)
        def _():
            pltpu.make_async_copy(source, target, term_recv.at[h, r]).wait()

        @pl.when(jnp.logical_not(from_self))
        def _():
            remote(source, target, term_send.at[h, r, 0], term_recv.at[h, r], (t, s)).wait_recv()

    spread, fanned, given = (slots.at[0, :, at(k * rows, rows)] for k in range(3))

    def cut(h):
        return at(h * lanes, lanes)

    def column_of(h):
        return at(s * rows + h * lanes, lanes)

    def swap_terms(h):
        return remote(landed.at[other, cut(h)], joined.at[:, cut(h)], pair_send.at[0, h], pair_recv.at[0, h], partner)

    def swap_states(h):
        return remote(given.at[:, cut(h)], got.at[:, cut(h)], pair_send.at[1, h], pair_recv.at[1, h], partner)

    def share_out(h, k):
        return remote(
            spread.at[at(k * share, share), cut(h)], gathered.at[pair, :, cut(h)],
            share_send.at[0, h, k], share_recv.at[0, h, pair], (core(2 * k, side), s),
        )

    def share_in(h, k):
        return remote(
            spread.at[at(k * share, share), cut(h)], gathered.at[k, :, cut(h)],
            share_send.at[0, h, k], share_recv.at[0, h, k], (core(2 * k, side), s),
        )

    def fan_out(h, k):
        return remote(
            fanned.at[at(k * share, share), cut(h)], evens.at[at(pair * share, share), cut(h)],
            share_send.at[1, h, k], share_recv.at[1, h, pair], (core(2 * k, side), s),
        )

    def fan_in(h, k):
        return remote(
            fanned.at[at(k * share, share), cut(h)], evens.at[at(k * share, share), cut(h)],
            share_send.at[1, h, k], share_recv.at[1, h, k], (core(2 * k, side), s),
        )

    def elsewhere(act):
        @pl.loop(0, pairs)
        def _(k):
            @pl.when(k != pair)
            def _():
                act(k)

    def solve(h):
        for r in range(pieces):
            wait_term(h, r)
        swap_terms(h).start()
        rate = coarse_decay(own, column_of(h))
        swap_terms(h).wait_recv()
        mine, theirs = landed[own, cut(h)], joined[:, cut(h)]
        first = jnp.where(side == 0, mine, theirs)
        second = jnp.where(side == 0, theirs, mine)
        spread[:, cut(h)] = second + jnp.where(pair == pairs - 1, 0.0, rate * first)
        elsewhere(lambda k: share_out(h, k).start())
        gathered[pair, :, cut(h)] = spread[at(pair * share, share), cut(h)]
        if h == 0:
            start_copy.wait()
        elsewhere(lambda k: share_in(h, k).wait_recv())
        near = coarse_decay(at(side * half + pair * share, share), column_of(h))
        value = gathered[pairs - 1, :, cut(h)] + near * start[:, cut(h)]
        fanned[0:share, cut(h)] = value
        near = near * near
        for k in range(pairs - 1):
            value = gathered[k, :, cut(h)] + near * value
            fanned[(k + 1) * share:(k + 2) * share, cut(h)] = value
        elsewhere(lambda k: fan_out(h, k).start())
        evens[at(pair * share, share), cut(h)] = fanned[at(pair * share, share), cut(h)]
        elsewhere(lambda k: fan_in(h, k).wait_recv())
        even = evens[:, cut(h)]
        odd = first + rate * even
        given[:, cut(h)] = jnp.where(side == 0, odd, even)
        swap_states(h).start()
        halves_to(tall, (own, cut(h)), jnp.where(side == 0, even, odd))
        swap_states(h).wait_recv()
        halves_to(tall, (other, cut(h)), got[:, cut(h)])

    def peer(k):
        return jnp.where(s < count // 2, count - 1 - k, k)

    def cross(stage, d, h, width, to, by):
        window = pl.ds(pl.multiple_of(d * rows + h * width, width), width)
        return remote(
            slots.at[stage + 1, 0:rows, window], crossed.at[stage, by, :, at(h * width, width)],
            cross_send.at[stage, d, h], cross_recv.at[stage, by, h], (to, d),
        )

    def dispatch(stage, h, width, block_for, to, keeps):
        @pl.loop(0, count)
        def _(k):
            d = peer(k)
            block = block_for(d)

            def away():
                slots[stage + 1, 0:rows, pl.ds(pl.multiple_of(d * rows + h * width, width), width)] = block
                cross(stage, d, h, width, to, s).start()

            if keeps:
                pl.when(d != s)(away)

                @pl.when(d == s)
                def _():
                    crossed[stage, s, :, at(h * width, width)] = block
            else:
                away()

    def absorb(stage, parts, width, use, keeps):
        if keeps:
            use(s, True)

        @pl.loop(0, count)
        def _(k):
            d = peer(k)

            def arrive(first):
                for h in range(parts):
                    cross(stage, d, h, width, t, d).wait_recv()
                use(d, first)

            if keeps:
                pl.when(d != s)(lambda: arrive(False))
            else:
                pl.when(k == 0)(lambda: arrive(True))
                pl.when(k != 0)(lambda: arrive(False))

    def left_rows(d, columns):
        return dot3((basis[0, span(d), :], basis[1, span(d), :]), (tall[0, :, columns], tall[1, :, columns]))

    def rows_into(ref, stage):
        def use(d, first):
            block = halves(crossed[stage, d])

            @pl.loop(0, 2)
            def _(n):
                columns = at(n * half, half)
                term = dot3(block, (basis_t[0, span(d), columns], basis_t[1, span(d), columns]))
                ref[:, columns] = term if first else ref[:, columns] + term
        return use

    for h in range(cuts):
        solve(h)
        dispatch(0, h, lanes, lambda d: left_rows(d, slice(h * lanes, (h + 1) * lanes)), t, True)

    absorb(0, cuts, lanes, rows_into(coarse_out, 0), True)
    moved = jnp.where(t == last, 0.0, reacted(coarse_out[...]))
    halves_to(wide, (slice(0, rows), slice(None)), moved + fine_next[...])

    dispatch(
        1, 0, rows,
        lambda d: dot3((wide[0, 0:rows, :], wide[1, 0:rows, :]), (basis[0, :, span(d)], basis[1, :, span(d)])), t, True,
    )

    def columns_use(d, first):
        block = halves(crossed[1, d])

        @pl.loop(0, 2)
        def _(r):
            lines = at(r * half, half)
            term = dot3((basis_t[0, lines, span(d)], basis_t[1, lines, span(d)]), block)
            kept[lines, 0:rows] = term if first else kept[lines, 0:rows] + term

    absorb(1, 1, rows, columns_use, True)

    @pl.loop(0, pieces)
    def _(r):
        block = at(r * piece, piece)
        halves_to(tall, (block, slice(0, rows)), kept[block, 0:rows] * fine_decay(block, span(s)))

    dispatch(2, 0, rows, lambda d: left_rows(d, slice(0, rows)), following, False)
    absorb(2, 1, rows, rows_into(fine_out, 2), False)

    @pl.when(holds)
    def _():
        leave_terms(cuts - 1)
        leave_home(coarse, 1)
        leave_home(fine_next, 2)

    leave_home(coarse_next, 3)

    @pl.when(t != last)
    def _():
        pass_guess(0).wait_send()
        pass_guess(1).wait_send()

    pass_fine.wait_send()
    pass_coarse.wait_send()
    for h in range(cuts):
        swap_terms(h).wait_send()
        swap_states(h).wait_send()
        elsewhere(lambda k: share_out(h, k).wait_send())
        elsewhere(lambda k: fan_out(h, k).wait_send())
    for stage, parts, width, to in ((0, cuts, lanes, t), (1, 1, rows, t), (2, 1, rows, following)):
        @pl.loop(0, count)
        def _(d):
            def leave():
                for h in range(parts):
                    cross(stage, d, h, width, to, s).wait_send()

            if stage == 2:
                leave()
            else:
                pl.when(d != s)(leave)


def on_device(initial, guess, fine, coarse, basis, rates, carried):
    grid, rows = basis.shape[0], initial.shape[0]
    half = grid // 2
    piece, count = half // 2, grid // rows
    per_half, pieces = count // 2, grid // piece
    steps, lanes = 7, 128
    cuts = rows // lanes
    pairs = lax.axis_size("tm") // 2
    share = half // pairs
    f32, bf16 = jnp.float32, jnp.bfloat16
    vmem, hbm = pl.BlockSpec(memory_space=pltpu.VMEM), pl.BlockSpec(memory_space=pltpu.HBM)
    dma = pltpu.SemaphoreType.DMA
    fine_new, coarse_new = pl.pallas_call(
        cycle_kernel,
        out_shape=[jax.ShapeDtypeStruct((rows, grid), f32)] * 2,
        in_specs=[hbm] * 6 + [vmem],
        out_specs=[vmem] * 2,
        scratch_shapes=[
            pltpu.VMEM((2, grid, grid), bf16),
            pltpu.VMEM((2, grid, grid), bf16),
            pltpu.VMEM((grid, lanes), f32),
            pltpu.VMEM((rows, grid), f32),
            pltpu.VMEM((rows, grid), f32),
            pltpu.VMEM((rows, grid), f32),
            pltpu.VMEM((rows, grid), f32),
            pltpu.VMEM((rows, grid), f32),
            pltpu.VMEM((4, half, grid), f32),
            pltpu.VMEM((half, grid), f32),
            pltpu.VMEM((grid, half), f32),
            pltpu.VMEM((grid, half), f32),
            pltpu.VMEM((2, half, grid), bf16),
            pltpu.VMEM((2, grid, half), bf16),
            pltpu.VMEM((2, half, half), bf16),
            pltpu.VMEM((2, half, half), f32),
            pltpu.VMEM((2, half, half), f32),
            pltpu.VMEM((grid, half), f32),
            pltpu.VMEM((grid, rows), f32),
            pltpu.VMEM((half, rows), f32),
            pltpu.VMEM((pairs, share, rows), f32),
            pltpu.VMEM((half, rows), f32),
            pltpu.VMEM((half, rows), f32),
            pltpu.VMEM((3, count, rows, rows), f32),
            pltpu.VMEM((share, rows), f32),
            dma((4, 2)),
            dma((4,)),
            dma((4,)),
            dma((4, count)),
            dma((steps, 2)),
            dma((steps, 2)),
            dma((cuts, pieces, per_half)),
            dma((cuts, pieces)),
            dma((2, cuts)),
            dma((2, cuts)),
            dma((2, cuts, pairs)),
            dma((2, cuts, pairs)),
            dma((3, count, cuts)),
            dma((3, count, cuts)),
            dma((5,)),
        ],
        compiler_params=pltpu.CompilerParams(has_side_effects=True, vmem_limit_bytes=54 * 1024 * 1024),
        cost_estimate=pl.CostEstimate(flops=200_000_000_000, bytes_accessed=16 * grid * grid, transcendentals=0),
        name="cycle",
    )(basis, guess[0], initial, fine[0], coarse[0], carried, rates[None, :])
    return fine_new[None], coarse_new[None]


def solution(mesh):
    placed = (
        P("space", None),
        P("tm", "space", None),
        P("tm", "space", None),
        P("tm", "space", None),
        P(),
        P(),
        P(),
    )
    return jax.shard_map(
        on_device,
        mesh=mesh,
        in_specs=placed,
        out_specs=(P("tm", "space", None), P("tm", "space", None)),
        check_vma=False,
    )
```

```python
import functools
import jax
import jax.numpy as jnp
from jax import lax
from jax.experimental import pallas as pl
from jax.experimental.pallas import tpu as pltpu
from jax.sharding import PartitionSpec as P

MESH = pl.DeviceIdType.MESH


def halves(block):
    high = block.astype(jnp.bfloat16)
    return high, (block - high.astype(jnp.float32)).astype(jnp.bfloat16)


def dot3(left, right):
    dot = functools.partial(jnp.dot, preferred_element_type=jnp.float32)
    return dot(left[0], right[0]) + dot(left[0], right[1]) + dot(left[1], right[0])


def reacted(value):
    return value + 0.5 * jnp.tanh(value)


def cycle_kernel(
    raw, guess, initial, fine, coarse, carried, rates, fine_out, coarse_out,
    basis, basis_t, rates_tall, fine_here, before, entry, fine_next, coarse_next, slots, field, coeffs, kept, wide, tall, part,
    sent, held, decay, landed, joined, gathered, evens, got, crossed, start,
    home_send, shift_send, shift_recv, slot_recv, ex_send, ex_recv, term_send, term_recv,
    pair_send, pair_recv, share_send, share_recv, cross_send, cross_recv, load_sem,
):
    groups, count = lax.axis_size("tm"), lax.axis_size("space")
    t, s = lax.axis_index("tm"), lax.axis_index("space")
    grid = raw.shape[0]
    rows = fine_here.shape[0]
    short = rows // 2
    half = grid // 2
    piece = half // 2
    pieces = grid // piece
    per_half = count // 2
    low_seat = per_half - 1
    last = groups - 1
    lanes = rates_tall.shape[1]
    cuts = rows // lanes
    pairs = groups // 2
    share = half // pairs

    def at(start, size):
        return pl.ds(pl.multiple_of(start, size), size)

    def span(d):
        return at(d * rows, rows)

    def seat(chain):
        return low_seat + chain % 2

    def core(chain, which):
        return 2 * (chain // 2) + which

    def remote(src, dst, send, recv, where):
        return pltpu.make_async_remote_copy(
            src_ref=src, dst_ref=dst, send_sem=send, recv_sem=recv,
            device_id={"tm": where[0], "space": where[1]}, device_id_type=MESH,
        )

    position = s % per_half
    group_at = (core(t, s // per_half), seat(t))
    to_self = (group_at[0] == t) & (group_at[1] == s)
    following, preceding = (t + 1) % groups, (t + groups - 1) % groups

    def group_copy(src, slot, k):
        part_of = src.at[at(k * short, short)]
        dst = slots.at[slot, at(position * rows + k * short, short)]
        return part_of, dst, home_send.at[slot, k], slot_recv.at[slot, 2 * position + k]

    def to_group(src, slot, k):
        part_of, dst, send, recv = group_copy(src, slot, k)

        @pl.when(jnp.logical_not(to_self))
        def _():
            remote(part_of, dst, send, recv, group_at).start()

        @pl.when(to_self)
        def _():
            pltpu.make_async_copy(part_of, dst, recv).start()

    def leave_home(src, slot):
        @pl.when(jnp.logical_not(to_self))
        def _():
            for k in range(2):
                remote(*group_copy(src, slot, k), group_at).wait_send()

    def pass_on(index, src, dst, where):
        return remote(src, dst, shift_send.at[index], shift_recv.at[index], (where, s))

    def pass_guess(k):
        lines = at(k * short, short)
        return pass_on(k, guess.at[lines], before.at[lines], following)

    pass_fine = pass_on(2, fine, fine_next, preceding)
    pass_entry = pass_on(2, entry, fine_next, preceding)
    pass_coarse = pass_on(3, coarse, coarse_next, preceding)

    side = t % 2
    pair = t // 2
    own, other = at(side * half, half), at((1 - side) * half, half)
    partner = (core(t, 1 - side), s)
    start_copy = pltpu.make_async_copy(
        carried.at[at(side * half + pair * share, share), span(s)], start, load_sem.at[0]
    )
    load_fine = pltpu.make_async_copy(fine, fine_here, load_sem.at[1])
    load_initial = pltpu.make_async_copy(initial, before, load_sem.at[2])
    load_low = pltpu.make_async_copy(raw.at[:, 0:half], coeffs, load_sem.at[3])
    load_high = pltpu.make_async_copy(raw.at[:, half:grid], kept, load_sem.at[4])

    @pl.when(t != last)
    def _():
        pass_guess(0).start()
        pass_guess(1).start()

    load_fine.start()

    @pl.when(t == 0)
    def _():
        load_initial.start()

    load_low.start()
    load_high.start()
    start_copy.start()

    @pl.when(t % 2 == 0)
    def _():
        to_group(coarse, 1, 0)

    load_fine.wait()

    @pl.when(t == 0)
    def _():
        load_initial.wait()

    for k in range(2):
        @pl.when(t != 0)
        def _():
            pass_guess(k).wait_recv()

        lines = at(k * short, short)
        entry[lines, :] = reacted(before[lines, :]) + fine_here[lines, :]
        to_group(entry, 0, k)

    @pl.when(t != 0)
    def _():
        pass_fine.start()

    load_low.wait()
    load_high.wait()
    for which, ref in enumerate((coeffs, kept)):
        @pl.loop(0, count)
        def _(r):
            high, low = halves(ref[span(r), :])
            basis[0, span(r), which * half:(which + 1) * half] = high
            basis[1, span(r), which * half:(which + 1) * half] = low

        @pl.loop(0, pieces)
        def _(c):
            for r in range(2):
                lines = slice(which * half + r * piece, which * half + (r + 1) * piece)
                high, low = halves(ref[at(c * piece, piece), r * piece:(r + 1) * piece].T)
                basis_t[0, lines, at(c * piece, piece)] = high
                basis_t[1, lines, at(c * piece, piece)] = low

    @pl.loop(0, grid // lanes)
    def _(r):
        rates_tall[at(r * lanes, lanes), :] = jnp.broadcast_to(rates[:, at(r * lanes, lanes)], (lanes, lanes)).T

    leave_home(entry, 0)

    @pl.when(t == 0)
    def _():
        pass_entry.start()

    @pl.when(t % 2 == 1)
    def _():
        to_group(coarse, 1, 0)

    to_group(coarse, 1, 1)
    pass_coarse.start()

    def home_fine():
        pass_fine.wait_recv()
        to_group(fine_next, 2, 0)
        to_group(fine_next, 2, 1)

    def home_coarse():
        pass_coarse.wait_recv()
        to_group(coarse_next, 3, 0)
        to_group(coarse_next, 3, 1)

    def sums_of_rates(block, columns):
        return rates_tall[block, :1] + rates[:, columns]

    def fine_decay(block, columns):
        return 1.0 / (1.0 + sums_of_rates(block, columns))

    def coarse_decay(block, columns):
        return 1.0 / (1.0 + 2.0 * sums_of_rates(block, columns))

    group = core(t, s - low_seat)

    def wait_slot(slot, index):
        local = (group == t) & (side * per_half + index == s)
        for k in range(2):
            dst = slots.at[slot, at(index * rows + k * short, short)]
            src, recv = entry.at[at(k * short, short)], slot_recv.at[slot, 2 * index + k]

            @pl.when(jnp.logical_not(local))
            def _():
                remote(src, dst, home_send.at[slot, k], recv, (t, s)).wait_recv()

            @pl.when(local)
            def _():
                pltpu.make_async_copy(src, dst, recv).wait()

    def exchange(stage, m):
        block = at(m * piece, piece)
        return remote(sent.at[stage % 2, block], held.at[stage % 2, block], ex_send.at[stage, m], ex_recv.at[stage, m], partner)

    def halves_to(ref, index, value):
        ref[(0, *index)], ref[(1, *index)] = halves(value)

    def reorder(value, order):
        if not order:
            return value
        return jnp.concatenate(
            [value[:, q * rows + h * lanes:q * rows + (h + 1) * lanes] for h in range(cuts) for q in range(per_half)], 1
        )

    def collect(stage, into, order=False):
        for m in range(2):
            block = at(m * piece, piece)
            exchange(stage, m).wait_recv()
            halves_to(into, (block, slice(0, half)), reorder(held[stage % 2, block, :], order))

    def free(stage):
        if stage >= 2:
            for m in range(2):
                exchange(stage - 2, m).wait_send()

    def right_of(stage, source, slot, order=False):
        free(stage)
        for m in range(2):
            block = at(m * piece, piece)
            for index in range(m * per_half // 2, (m + 1) * per_half // 2):
                wait_slot(slot, index)
            halves_to(wide, (block, slice(None)), source(block))
            left = (wide[0, block, :], wide[1, block, :])
            sent[stage % 2, block] = dot3(left, (basis[0, :, other], basis[1, :, other]))
            exchange(stage, m).start()
            halves_to(part, (block, slice(None)), reorder(dot3(left, (basis[0, :, own], basis[1, :, own])), order))

    def forward(stage, source, slot, finish):
        right_of(stage, source, slot)

        @pl.loop(0, 2)
        def _(n):
            columns = at(n * piece, piece)
            coeffs[:, columns] = dot3((basis_t[0, :, own], basis_t[1, :, own]), (part[0, :, columns], part[1, :, columns]))

        collect(stage, part)

        @pl.loop(0, 2)
        def _(n):
            columns = at(n * piece, piece)
            term = dot3((basis_t[0, :, other], basis_t[1, :, other]), (part[0, :, columns], part[1, :, columns]))
            value = (coeffs[:, columns] + term) * decay[:, columns]
            coeffs[:, columns] = value
            finish(n, columns, value)

    def inverse(stage, midway=None):
        free(stage)

        @pl.loop(0, pieces)
        def _(r):
            block = at(r * piece, piece)
            halves_to(tall, (block, slice(None)), coeffs[block, :])

        def rows_of(m, which):
            block = at(which * half + m * piece, piece)
            return dot3((basis[0, block, :], basis[1, block, :]), (tall[0], tall[1]))

        @pl.loop(0, 2)
        def _(m):
            sent[stage % 2, at(m * piece, piece)] = rows_of(m, 1 - side)
            exchange(stage, m).start()

        @pl.loop(0, 2)
        def _(m):
            halves_to(part, (at(m * piece, piece), slice(None)), rows_of(m, side))

        if midway is not None:
            midway()

        @pl.loop(0, 2)
        def _(n):
            columns = at(n * half, half)
            field[:, columns] = dot3((part[0], part[1]), (basis_t[0, own, columns], basis_t[1, own, columns]))

        collect(stage, part)

        @pl.loop(0, 2)
        def _(n):
            columns = at(n * half, half)
            field[:, columns] = field[:, columns] + dot3(
                (part[0], part[1]), (basis_t[0, other, columns], basis_t[1, other, columns])
            )

    def term_place(q):
        return group, side * per_half + q

    def term_refs(h, r, q):
        block = at(r * piece, piece)
        source = coeffs.at[block, at((h * per_half + q) * lanes, lanes)]
        return source, landed.at[block, at(h * lanes, lanes)]

    def term_here(q):
        where = term_place(q)
        return (where[0] == t) & (where[1] == s)

    def send_term(h, r, q):
        source, target = term_refs(h, r, q)

        @pl.when(term_here(q))
        def _():
            pltpu.make_async_copy(source, target, term_recv.at[h, r]).start()

        @pl.when(jnp.logical_not(term_here(q)))
        def _():
            remote(source, target, term_send.at[h, r, q], term_recv.at[h, r], term_place(q)).start()

    def leave_terms(h):
        for q in range(per_half):
            @pl.when(jnp.logical_not(term_here(q)))
            def _():
                for r in range(pieces):
                    source, target = term_refs(h, r, q)
                    remote(source, target, term_send.at[h, r, q], term_recv.at[h, r], term_place(q)).wait_send()

    holds = (s == low_seat) | (s == low_seat + 1)

    @pl.when(jnp.logical_not(holds))
    def _():
        leave_home(coarse, 1)
        home_fine()
        leave_home(fine_next, 2)
        home_coarse()

    @pl.when(holds)
    def _():
        @pl.loop(0, pieces)
        def _(r):
            block = at(r * piece, piece)
            decay[block, :] = fine_decay(block, own)

        def plain(n, columns, value):
            pass

        def keep(n, columns, value):
            taken = value * coarse_decay(slice(None), at(side * half + n * piece, piece))
            kept[:, columns] = jnp.where(group == last, 0.0, taken)

        def from_field(slot):
            def source(block):
                moved = reacted(field[block, :])
                if slot == 2:
                    moved = jnp.where(group == last, 0.0, moved)
                return moved + slots[slot, block, :]
            return source

        forward(0, lambda block: slots[0, block, :], 0, plain)
        home_fine()
        inverse(1)
        forward(2, from_field(1), 1, keep)
        inverse(3, home_coarse)
        forward(4, from_field(2), 2, plain)
        inverse(5)

        right_of(6, from_field(3), 3, True)
        collect(6, wide, True)
        for h in range(cuts):
            columns = slice(h * per_half * lanes, (h + 1) * per_half * lanes)

            @pl.loop(0, pieces)
            def _(r):
                block = at(r * piece, piece)
                value = dot3((basis_t[0, block, own], basis_t[1, block, own]), (part[0, :, columns], part[1, :, columns]))
                value = value + dot3(
                    (basis_t[0, block, other], basis_t[1, block, other]), (wide[0, :, columns], wide[1, :, columns])
                )
                for q in range(per_half):
                    natural = slice(q * rows + h * lanes, q * rows + (h + 1) * lanes)
                    coeffs[block, at((h * per_half + q) * lanes, lanes)] = (
                        value[:, q * lanes:(q + 1) * lanes] * decay[block, natural] - kept[block, natural]
                    )
                if h == 0:
                    for q in range(per_half):
                        send_term(h, r, q)

            if h > 0:
                leave_terms(h - 1)
                for r in range(pieces):
                    for q in range(per_half):
                        send_term(h, r, q)

        for stage in (5, 6):
            for m in range(2):
                exchange(stage, m).wait_send()

    sender = (core(t, s // per_half), seat(t))
    from_self = (sender[0] == t) & (sender[1] == s)

    def wait_term(h, r):
        source, target = term_refs(h, r, 0)

        @pl.when(from_self)
        def _():
            pltpu.make_async_copy(source, target, term_recv.at[h, r]).wait()

        @pl.when(jnp.logical_not(from_self))
        def _():
            remote(source, target, term_send.at[h, r, 0], term_recv.at[h, r], (t, s)).wait_recv()

    spread, fanned, given = (slots.at[0, :, at(k * rows, rows)] for k in range(3))

    def cut(h):
        return at(h * lanes, lanes)

    def column_of(h):
        return at(s * rows + h * lanes, lanes)

    def swap_terms(h):
        return remote(landed.at[other, cut(h)], joined.at[:, cut(h)], pair_send.at[0, h], pair_recv.at[0, h], partner)

    def swap_states(h):
        return remote(given.at[:, cut(h)], got.at[:, cut(h)], pair_send.at[1, h], pair_recv.at[1, h], partner)

    def share_out(h, k):
        return remote(
            spread.at[at(k * share, share), cut(h)], gathered.at[pair, :, cut(h)],
            share_send.at[0, h, k], share_recv.at[0, h, pair], (core(2 * k, side), s),
        )

    def share_in(h, k):
        return remote(
            spread.at[at(k * share, share), cut(h)], gathered.at[k, :, cut(h)],
            share_send.at[0, h, k], share_recv.at[0, h, k], (core(2 * k, side), s),
        )

    def fan_out(h, k):
        return remote(
            fanned.at[at(k * share, share), cut(h)], evens.at[at(pair * share, share), cut(h)],
            share_send.at[1, h, k], share_recv.at[1, h, pair], (core(2 * k, side), s),
        )

    def fan_in(h, k):
        return remote(
            fanned.at[at(k * share, share), cut(h)], evens.at[at(k * share, share), cut(h)],
            share_send.at[1, h, k], share_recv.at[1, h, k], (core(2 * k, side), s),
        )

    def elsewhere(act):
        @pl.loop(0, pairs)
        def _(k):
            @pl.when(k != pair)
            def _():
                act(k)

    def solve(h):
        for r in range(pieces):
            wait_term(h, r)
        swap_terms(h).start()
        rate = coarse_decay(own, column_of(h))
        swap_terms(h).wait_recv()
        mine, theirs = landed[own, cut(h)], joined[:, cut(h)]
        first = jnp.where(side == 0, mine, theirs)
        second = jnp.where(side == 0, theirs, mine)
        spread[:, cut(h)] = second + jnp.where(pair == pairs - 1, 0.0, rate * first)
        elsewhere(lambda k: share_out(h, k).start())
        gathered[pair, :, cut(h)] = spread[at(pair * share, share), cut(h)]
        if h == 0:
            start_copy.wait()
        elsewhere(lambda k: share_in(h, k).wait_recv())
        near = coarse_decay(at(side * half + pair * share, share), column_of(h))
        value = gathered[pairs - 1, :, cut(h)] + near * start[:, cut(h)]
        fanned[0:share, cut(h)] = value
        near = near * near
        for k in range(pairs - 1):
            value = gathered[k, :, cut(h)] + near * value
            fanned[(k + 1) * share:(k + 2) * share, cut(h)] = value
        elsewhere(lambda k: fan_out(h, k).start())
        evens[at(pair * share, share), cut(h)] = fanned[at(pair * share, share), cut(h)]
        elsewhere(lambda k: fan_in(h, k).wait_recv())
        even = evens[:, cut(h)]
        odd = first + rate * even
        given[:, cut(h)] = jnp.where(side == 0, odd, even)
        swap_states(h).start()
        halves_to(tall, (own, cut(h)), jnp.where(side == 0, even, odd))
        swap_states(h).wait_recv()
        halves_to(tall, (other, cut(h)), got[:, cut(h)])

    def peer(k):
        return jnp.where(s < count // 2, count - 1 - k, k)

    def cross(stage, d, h, width, to, by):
        window = pl.ds(pl.multiple_of(d * rows + h * width, width), width)
        return remote(
            slots.at[stage + 1, 0:rows, window], crossed.at[stage, by, :, at(h * width, width)],
            cross_send.at[stage, d, h], cross_recv.at[stage, by, h], (to, d),
        )

    def dispatch(stage, h, width, block_for, to, keeps):
        @pl.loop(0, count)
        def _(k):
            d = peer(k)
            block = block_for(d)

            def away():
                slots[stage + 1, 0:rows, pl.ds(pl.multiple_of(d * rows + h * width, width), width)] = block
                cross(stage, d, h, width, to, s).start()

            if keeps:
                pl.when(d != s)(away)

                @pl.when(d == s)
                def _():
                    crossed[stage, s, :, at(h * width, width)] = block
            else:
                away()

    def absorb(stage, parts, width, use, keeps):
        if keeps:
            use(s, True)

        @pl.loop(0, count)
        def _(k):
            d = peer(k)

            def arrive(first):
                for h in range(parts):
                    cross(stage, d, h, width, t, d).wait_recv()
                use(d, first)

            if keeps:
                pl.when(d != s)(lambda: arrive(False))
            else:
                pl.when(k == 0)(lambda: arrive(True))
                pl.when(k != 0)(lambda: arrive(False))

    def left_rows(d, columns):
        return dot3((basis[0, span(d), :], basis[1, span(d), :]), (tall[0, :, columns], tall[1, :, columns]))

    def rows_into(ref, stage):
        def use(d, first):
            block = halves(crossed[stage, d])

            @pl.loop(0, 2)
            def _(n):
                columns = at(n * half, half)
                term = dot3(block, (basis_t[0, span(d), columns], basis_t[1, span(d), columns]))
                ref[:, columns] = term if first else ref[:, columns] + term
        return use

    for h in range(cuts):
        solve(h)
        dispatch(0, h, lanes, lambda d: left_rows(d, slice(h * lanes, (h + 1) * lanes)), t, True)

    absorb(0, cuts, lanes, rows_into(coarse_out, 0), True)
    moved = jnp.where(t == last, 0.0, reacted(coarse_out[...]))
    halves_to(wide, (slice(0, rows), slice(None)), moved + fine_next[...])

    dispatch(
        1, 0, rows,
        lambda d: dot3((wide[0, 0:rows, :], wide[1, 0:rows, :]), (basis[0, :, span(d)], basis[1, :, span(d)])), t, True,
    )

    def columns_use(d, first):
        block = halves(crossed[1, d])

        @pl.loop(0, 2)
        def _(r):
            lines = at(r * half, half)
            term = dot3((basis_t[0, lines, span(d)], basis_t[1, lines, span(d)]), block)
            kept[lines, 0:rows] = term if first else kept[lines, 0:rows] + term

    absorb(1, 1, rows, columns_use, True)

    @pl.loop(0, pieces)
    def _(r):
        block = at(r * piece, piece)
        halves_to(tall, (block, slice(0, rows)), kept[block, 0:rows] * fine_decay(block, span(s)))

    dispatch(2, 0, rows, lambda d: left_rows(d, slice(0, rows)), following, False)
    absorb(2, 1, rows, rows_into(fine_out, 2), False)

    @pl.when(holds)
    def _():
        leave_terms(cuts - 1)
        leave_home(coarse, 1)
        leave_home(fine_next, 2)

    leave_home(coarse_next, 3)

    @pl.when(t != last)
    def _():
        pass_guess(0).wait_send()
        pass_guess(1).wait_send()

    pass_fine.wait_send()
    pass_coarse.wait_send()
    for h in range(cuts):
        swap_terms(h).wait_send()
        swap_states(h).wait_send()
        elsewhere(lambda k: share_out(h, k).wait_send())
        elsewhere(lambda k: fan_out(h, k).wait_send())
    for stage, parts, width, to in ((0, cuts, lanes, t), (1, 1, rows, t), (2, 1, rows, following)):
        @pl.loop(0, count)
        def _(d):
            def leave():
                for h in range(parts):
                    cross(stage, d, h, width, to, s).wait_send()

            if stage == 2:
                leave()
            else:
                pl.when(d != s)(leave)


def on_device(initial, guess, fine, coarse, basis, rates, carried):
    grid, rows = basis.shape[0], initial.shape[0]
    half = grid // 2
    piece, count = half // 2, grid // rows
    per_half, pieces = count // 2, grid // piece
    steps, lanes = 7, 128
    cuts = rows // lanes
    pairs = lax.axis_size("tm") // 2
    share = half // pairs
    f32, bf16 = jnp.float32, jnp.bfloat16
    vmem, hbm = pl.BlockSpec(memory_space=pltpu.VMEM), pl.BlockSpec(memory_space=pltpu.HBM)
    dma = pltpu.SemaphoreType.DMA
    fine_new, coarse_new = pl.pallas_call(
        cycle_kernel,
        out_shape=[jax.ShapeDtypeStruct((rows, grid), f32)] * 2,
        in_specs=[hbm] * 6 + [vmem],
        out_specs=[vmem] * 2,
        scratch_shapes=[
            pltpu.VMEM((2, grid, grid), bf16),
            pltpu.VMEM((2, grid, grid), bf16),
            pltpu.VMEM((grid, lanes), f32),
            pltpu.VMEM((rows, grid), f32),
            pltpu.VMEM((rows, grid), f32),
            pltpu.VMEM((rows, grid), f32),
            pltpu.VMEM((rows, grid), f32),
            pltpu.VMEM((rows, grid), f32),
            pltpu.VMEM((4, half, grid), f32),
            pltpu.VMEM((half, grid), f32),
            pltpu.VMEM((grid, half), f32),
            pltpu.VMEM((grid, half), f32),
            pltpu.VMEM((2, half, grid), bf16),
            pltpu.VMEM((2, grid, half), bf16),
            pltpu.VMEM((2, half, half), bf16),
            pltpu.VMEM((2, half, half), f32),
            pltpu.VMEM((2, half, half), f32),
            pltpu.VMEM((grid, half), f32),
            pltpu.VMEM((grid, rows), f32),
            pltpu.VMEM((half, rows), f32),
            pltpu.VMEM((pairs, share, rows), f32),
            pltpu.VMEM((half, rows), f32),
            pltpu.VMEM((half, rows), f32),
            pltpu.VMEM((3, count, rows, rows), f32),
            pltpu.VMEM((share, rows), f32),
            dma((4, 2)),
            dma((4,)),
            dma((4,)),
            dma((4, count)),
            dma((steps, 2)),
            dma((steps, 2)),
            dma((cuts, pieces, per_half)),
            dma((cuts, pieces)),
            dma((2, cuts)),
            dma((2, cuts)),
            dma((2, cuts, pairs)),
            dma((2, cuts, pairs)),
            dma((3, count, cuts)),
            dma((3, count, cuts)),
            dma((5,)),
        ],
        compiler_params=pltpu.CompilerParams(has_side_effects=True, vmem_limit_bytes=50 * 1024 * 1024),
        cost_estimate=pl.CostEstimate(flops=200_000_000_000, bytes_accessed=16 * grid * grid, transcendentals=0),
        name="cycle",
    )(basis, guess[0], initial, fine[0], coarse[0], carried, rates[None, :])
    return fine_new[None], coarse_new[None]


def solution(mesh):
    placed = (
        P("space", None),
        P("tm", "space", None),
        P("tm", "space", None),
        P("tm", "space", None),
        P(),
        P(),
        P(),
    )
    return jax.shard_map(
        on_device,
        mesh=mesh,
        in_specs=placed,
        out_specs=(P("tm", "space", None), P("tm", "space", None)),
        check_vma=False,
    )
```

```python
import functools
import jax
import jax.numpy as jnp
from jax import lax
from jax.experimental import pallas as pl
from jax.experimental.pallas import tpu as pltpu
from jax.sharding import PartitionSpec as P

MESH = pl.DeviceIdType.MESH


def halves(block):
    high = block.astype(jnp.bfloat16)
    return high, (block - high.astype(jnp.float32)).astype(jnp.bfloat16)


def dot3(left, right):
    dot = functools.partial(jnp.dot, preferred_element_type=jnp.float32)
    return dot(left[0], right[0]) + dot(left[0], right[1]) + dot(left[1], right[0])


def reacted(value):
    return value + 0.5 * jnp.tanh(value)


def cycle_kernel(
    raw, guess, initial, fine, coarse, carried, rates, fine_out, coarse_out,
    basis, basis_t, rates_tall, fine_here, before, entry, fine_next, coarse_next, slots, field, coeffs, kept, wide, tall, part,
    sent, held, decay, landed, joined, gathered, evens, got, crossed, start,
    home_send, shift_send, shift_recv, slot_recv, ex_send, ex_recv, term_send, term_recv,
    pair_send, pair_recv, share_send, share_recv, cross_send, cross_recv, load_sem,
):
    groups, count = lax.axis_size("tm"), lax.axis_size("space")
    t, s = lax.axis_index("tm"), lax.axis_index("space")
    grid = raw.shape[0]
    rows = fine_here.shape[0]
    short = rows // 2
    half = grid // 2
    piece = half // 2
    pieces = grid // piece
    per_half = count // 2
    low_seat = per_half - 1
    last = groups - 1
    lanes = rates_tall.shape[1]
    cuts = rows // lanes
    pairs = groups // 2
    share = half // pairs

    def at(start, size):
        return pl.ds(pl.multiple_of(start, size), size)

    def span(d):
        return at(d * rows, rows)

    def seat(chain):
        return low_seat + chain % 2

    def core(chain, which):
        return 2 * (chain // 2) + which

    def remote(src, dst, send, recv, where):
        return pltpu.make_async_remote_copy(
            src_ref=src, dst_ref=dst, send_sem=send, recv_sem=recv,
            device_id={"tm": where[0], "space": where[1]}, device_id_type=MESH,
        )

    position = s % per_half
    group_at = (core(t, s // per_half), seat(t))
    to_self = (group_at[0] == t) & (group_at[1] == s)
    following, preceding = (t + 1) % groups, (t + groups - 1) % groups

    def group_copy(src, slot, k):
        part_of = src.at[at(k * short, short)]
        dst = slots.at[slot, at(position * rows + k * short, short)]
        return part_of, dst, home_send.at[slot, k], slot_recv.at[slot, 2 * position + k]

    def to_group(src, slot, k):
        part_of, dst, send, recv = group_copy(src, slot, k)

        @pl.when(jnp.logical_not(to_self))
        def _():
            remote(part_of, dst, send, recv, group_at).start()

        @pl.when(to_self)
        def _():
            pltpu.make_async_copy(part_of, dst, recv).start()

    def leave_home(src, slot):
        @pl.when(jnp.logical_not(to_self))
        def _():
            for k in range(2):
                remote(*group_copy(src, slot, k), group_at).wait_send()

    def pass_on(index, src, dst, where):
        return remote(src, dst, shift_send.at[index], shift_recv.at[index], (where, s))

    def pass_guess(k):
        lines = at(k * short, short)
        return pass_on(k, guess.at[lines], before.at[lines], following)

    pass_fine = pass_on(2, fine, fine_next, preceding)
    pass_entry = pass_on(2, entry, fine_next, preceding)
    pass_coarse = pass_on(3, coarse, coarse_next, preceding)

    side = t % 2
    pair = t // 2
    own, other = at(side * half, half), at((1 - side) * half, half)
    partner = (core(t, 1 - side), s)
    start_copy = pltpu.make_async_copy(
        carried.at[at(side * half + pair * share, share), span(s)], start, load_sem.at[0]
    )
    load_fine = pltpu.make_async_copy(fine, fine_here, load_sem.at[1])
    load_initial = pltpu.make_async_copy(initial, before, load_sem.at[2])
    load_low = pltpu.make_async_copy(raw.at[:, 0:half], coeffs, load_sem.at[3])
    load_high = pltpu.make_async_copy(raw.at[:, half:grid], kept, load_sem.at[4])

    @pl.when(t != last)
    def _():
        pass_guess(0).start()
        pass_guess(1).start()

    load_fine.start()

    @pl.when(t == 0)
    def _():
        load_initial.start()

    load_low.start()
    load_high.start()
    start_copy.start()

    @pl.when(t % 2 == 0)
    def _():
        to_group(coarse, 1, 0)

    load_fine.wait()

    @pl.when(t == 0)
    def _():
        load_initial.wait()

    for k in range(2):
        @pl.when(t != 0)
        def _():
            pass_guess(k).wait_recv()

        lines = at(k * short, short)
        entry[lines, :] = reacted(before[lines, :]) + fine_here[lines, :]
        to_group(entry, 0, k)

    @pl.when(t != 0)
    def _():
        pass_fine.start()

    load_low.wait()
    load_high.wait()
    for which, ref in enumerate((coeffs, kept)):
        @pl.loop(0, count)
        def _(r):
            high, low = halves(ref[span(r), :])
            basis[0, span(r), which * half:(which + 1) * half] = high
            basis[1, span(r), which * half:(which + 1) * half] = low

        @pl.loop(0, pieces)
        def _(c):
            for r in range(2):
                lines = slice(which * half + r * piece, which * half + (r + 1) * piece)
                high, low = halves(ref[at(c * piece, piece), r * piece:(r + 1) * piece].T)
                basis_t[0, lines, at(c * piece, piece)] = high
                basis_t[1, lines, at(c * piece, piece)] = low

    @pl.loop(0, grid // lanes)
    def _(r):
        rates_tall[at(r * lanes, lanes), :] = jnp.broadcast_to(rates[:, at(r * lanes, lanes)], (lanes, lanes)).T

    leave_home(entry, 0)

    @pl.when(t == 0)
    def _():
        pass_entry.start()

    @pl.when(t % 2 == 1)
    def _():
        to_group(coarse, 1, 0)

    to_group(coarse, 1, 1)
    pass_coarse.start()

    def home_fine():
        pass_fine.wait_recv()
        to_group(fine_next, 2, 0)
        to_group(fine_next, 2, 1)

    def home_coarse():
        pass_coarse.wait_recv()
        to_group(coarse_next, 3, 0)
        to_group(coarse_next, 3, 1)

    def sums_of_rates(block, columns):
        return rates_tall[block, :1] + rates[:, columns]

    def fine_decay(block, columns):
        return 1.0 / (1.0 + sums_of_rates(block, columns))

    def coarse_decay(block, columns):
        return 1.0 / (1.0 + 2.0 * sums_of_rates(block, columns))

    group = core(t, s - low_seat)

    def wait_slot(slot, index):
        local = (group == t) & (side * per_half + index == s)
        for k in range(2):
            dst = slots.at[slot, at(index * rows + k * short, short)]
            src, recv = entry.at[at(k * short, short)], slot_recv.at[slot, 2 * index + k]

            @pl.when(jnp.logical_not(local))
            def _():
                remote(src, dst, home_send.at[slot, k], recv, (t, s)).wait_recv()

            @pl.when(local)
            def _():
                pltpu.make_async_copy(src, dst, recv).wait()

    def exchange(stage, m):
        block = at(m * piece, piece)
        return remote(sent.at[stage % 2, block], held.at[stage % 2, block], ex_send.at[stage, m], ex_recv.at[stage, m], partner)

    def halves_to(ref, index, value):
        ref[(0, *index)], ref[(1, *index)] = halves(value)

    def reorder(value, order):
        if not order:
            return value
        return jnp.concatenate(
            [value[:, q * rows + h * lanes:q * rows + (h + 1) * lanes] for h in range(cuts) for q in range(per_half)], 1
        )

    def collect(stage, into, order=False):
        for m in range(2):
            block = at(m * piece, piece)
            exchange(stage, m).wait_recv()
            halves_to(into, (block, slice(0, half)), reorder(held[stage % 2, block, :], order))

    def free(stage):
        if stage >= 2:
            for m in range(2):
                exchange(stage - 2, m).wait_send()

    def right_of(stage, source, slot, order=False):
        free(stage)
        for m in range(2):
            block = at(m * piece, piece)
            for index in range(m * per_half // 2, (m + 1) * per_half // 2):
                wait_slot(slot, index)
            halves_to(wide, (block, slice(None)), source(block))
            left = (wide[0, block, :], wide[1, block, :])
            sent[stage % 2, block] = dot3(left, (basis[0, :, other], basis[1, :, other]))
            exchange(stage, m).start()
            halves_to(part, (block, slice(None)), reorder(dot3(left, (basis[0, :, own], basis[1, :, own])), order))

    def forward(stage, source, slot, finish):
        right_of(stage, source, slot)

        @pl.loop(0, 2)
        def _(n):
            columns = at(n * piece, piece)
            coeffs[:, columns] = dot3((basis_t[0, :, own], basis_t[1, :, own]), (part[0, :, columns], part[1, :, columns]))

        collect(stage, part)

        @pl.loop(0, 2)
        def _(n):
            columns = at(n * piece, piece)
            term = dot3((basis_t[0, :, other], basis_t[1, :, other]), (part[0, :, columns], part[1, :, columns]))
            value = (coeffs[:, columns] + term) * decay[:, columns]
            coeffs[:, columns] = value
            finish(n, columns, value)

    def inverse(stage, midway=None):
        free(stage)

        @pl.loop(0, pieces)
        def _(r):
            block = at(r * piece, piece)
            halves_to(tall, (block, slice(None)), coeffs[block, :])

        def rows_of(m, which):
            block = at(which * half + m * piece, piece)
            return dot3((basis[0, block, :], basis[1, block, :]), (tall[0], tall[1]))

        @pl.loop(0, 2)
        def _(m):
            sent[stage % 2, at(m * piece, piece)] = rows_of(m, 1 - side)
            exchange(stage, m).start()

        @pl.loop(0, 2)
        def _(m):
            halves_to(part, (at(m * piece, piece), slice(None)), rows_of(m, side))

        if midway is not None:
            midway()

        @pl.loop(0, 2)
        def _(n):
            columns = at(n * half, half)
            field[:, columns] = dot3((part[0], part[1]), (basis_t[0, own, columns], basis_t[1, own, columns]))

        collect(stage, part)

        @pl.loop(0, 2)
        def _(n):
            columns = at(n * half, half)
            field[:, columns] = field[:, columns] + dot3(
                (part[0], part[1]), (basis_t[0, other, columns], basis_t[1, other, columns])
            )

    def term_place(q):
        return group, side * per_half + q

    def term_refs(h, r, q):
        block = at(r * piece, piece)
        source = coeffs.at[block, at((h * per_half + q) * lanes, lanes)]
        return source, landed.at[block, at(h * lanes, lanes)]

    def term_here(q):
        where = term_place(q)
        return (where[0] == t) & (where[1] == s)

    def send_term(h, r, q):
        source, target = term_refs(h, r, q)

        @pl.when(term_here(q))
        def _():
            pltpu.make_async_copy(source, target, term_recv.at[h, r]).start()

        @pl.when(jnp.logical_not(term_here(q)))
        def _():
            remote(source, target, term_send.at[h, r, q], term_recv.at[h, r], term_place(q)).start()

    def leave_terms(h):
        for q in range(per_half):
            @pl.when(jnp.logical_not(term_here(q)))
            def _():
                for r in range(pieces):
                    source, target = term_refs(h, r, q)
                    remote(source, target, term_send.at[h, r, q], term_recv.at[h, r], term_place(q)).wait_send()

    holds = (s == low_seat) | (s == low_seat + 1)

    @pl.when(jnp.logical_not(holds))
    def _():
        leave_home(coarse, 1)
        home_fine()
        leave_home(fine_next, 2)
        home_coarse()

    @pl.when(holds)
    def _():
        @pl.loop(0, pieces)
        def _(r):
            block = at(r * piece, piece)
            decay[block, :] = fine_decay(block, own)

        def plain(n, columns, value):
            pass

        def keep(n, columns, value):
            taken = value * coarse_decay(slice(None), at(side * half + n * piece, piece))
            kept[:, columns] = jnp.where(group == last, 0.0, taken)

        def from_field(slot):
            def source(block):
                moved = reacted(field[block, :])
                if slot == 2:
                    moved = jnp.where(group == last, 0.0, moved)
                return moved + slots[slot, block, :]
            return source

        forward(0, lambda block: slots[0, block, :], 0, plain)
        home_fine()
        inverse(1)
        forward(2, from_field(1), 1, keep)
        inverse(3, home_coarse)
        forward(4, from_field(2), 2, plain)
        inverse(5)

        right_of(6, from_field(3), 3, True)
        collect(6, wide, True)
        for h in range(cuts):
            columns = slice(h * per_half * lanes, (h + 1) * per_half * lanes)

            @pl.loop(0, pieces)
            def _(r):
                block = at(r * piece, piece)
                value = dot3((basis_t[0, block, own], basis_t[1, block, own]), (part[0, :, columns], part[1, :, columns]))
                value = value + dot3(
                    (basis_t[0, block, other], basis_t[1, block, other]), (wide[0, :, columns], wide[1, :, columns])
                )
                for q in range(per_half):
                    natural = slice(q * rows + h * lanes, q * rows + (h + 1) * lanes)
                    coeffs[block, at((h * per_half + q) * lanes, lanes)] = (
                        value[:, q * lanes:(q + 1) * lanes] * decay[block, natural] - kept[block, natural]
                    )
                if h == 0:
                    for q in range(per_half):
                        send_term(h, r, q)

            if h > 0:
                leave_terms(h - 1)
                for r in range(pieces):
                    for q in range(per_half):
                        send_term(h, r, q)

        for stage in (5, 6):
            for m in range(2):
                exchange(stage, m).wait_send()

    sender = (core(t, s // per_half), seat(t))
    from_self = (sender[0] == t) & (sender[1] == s)

    def wait_term(h, r):
        source, target = term_refs(h, r, 0)

        @pl.when(from_self)
        def _():
            pltpu.make_async_copy(source, target, term_recv.at[h, r]).wait()

        @pl.when(jnp.logical_not(from_self))
        def _():
            remote(source, target, term_send.at[h, r, 0], term_recv.at[h, r], (t, s)).wait_recv()

    spread, fanned, given = (slots.at[0, :, at(k * rows, rows)] for k in range(3))

    def cut(h):
        return at(h * lanes, lanes)

    def column_of(h):
        return at(s * rows + h * lanes, lanes)

    def swap_terms(h):
        return remote(landed.at[other, cut(h)], joined.at[:, cut(h)], pair_send.at[0, h], pair_recv.at[0, h], partner)

    def swap_states(h):
        return remote(given.at[:, cut(h)], got.at[:, cut(h)], pair_send.at[1, h], pair_recv.at[1, h], partner)

    def share_out(h, k):
        return remote(
            spread.at[at(k * share, share), cut(h)], gathered.at[pair, :, cut(h)],
            share_send.at[0, h, k], share_recv.at[0, h, pair], (core(2 * k, side), s),
        )

    def share_in(h, k):
        return remote(
            spread.at[at(k * share, share), cut(h)], gathered.at[k, :, cut(h)],
            share_send.at[0, h, k], share_recv.at[0, h, k], (core(2 * k, side), s),
        )

    def fan_out(h, k):
        return remote(
            fanned.at[at(k * share, share), cut(h)], evens.at[at(pair * share, share), cut(h)],
            share_send.at[1, h, k], share_recv.at[1, h, pair], (core(2 * k, side), s),
        )

    def fan_in(h, k):
        return remote(
            fanned.at[at(k * share, share), cut(h)], evens.at[at(k * share, share), cut(h)],
            share_send.at[1, h, k], share_recv.at[1, h, k], (core(2 * k, side), s),
        )

    def elsewhere(act):
        @pl.loop(0, pairs)
        def _(k):
            @pl.when(k != pair)
            def _():
                act(k)

    def solve(h):
        for r in range(pieces):
            wait_term(h, r)
        swap_terms(h).start()
        rate = coarse_decay(own, column_of(h))
        swap_terms(h).wait_recv()
        mine, theirs = landed[own, cut(h)], joined[:, cut(h)]
        first = jnp.where(side == 0, mine, theirs)
        second = jnp.where(side == 0, theirs, mine)
        spread[:, cut(h)] = second + jnp.where(pair == pairs - 1, 0.0, rate * first)
        elsewhere(lambda k: share_out(h, k).start())
        gathered[pair, :, cut(h)] = spread[at(pair * share, share), cut(h)]
        if h == 0:
            start_copy.wait()
        elsewhere(lambda k: share_in(h, k).wait_recv())
        near = coarse_decay(at(side * half + pair * share, share), column_of(h))
        value = gathered[pairs - 1, :, cut(h)] + near * start[:, cut(h)]
        fanned[0:share, cut(h)] = value
        near = near * near
        for k in range(pairs - 1):
            value = gathered[k, :, cut(h)] + near * value
            fanned[(k + 1) * share:(k + 2) * share, cut(h)] = value
        elsewhere(lambda k: fan_out(h, k).start())
        evens[at(pair * share, share), cut(h)] = fanned[at(pair * share, share), cut(h)]
        elsewhere(lambda k: fan_in(h, k).wait_recv())
        even = evens[:, cut(h)]
        odd = first + rate * even
        given[:, cut(h)] = jnp.where(side == 0, odd, even)
        swap_states(h).start()
        halves_to(tall, (own, cut(h)), jnp.where(side == 0, even, odd))
        swap_states(h).wait_recv()
        halves_to(tall, (other, cut(h)), got[:, cut(h)])

    def peer(k):
        return jnp.where(s < count // 2, count - 1 - k, k)

    thin = [(0, rows, h * lanes, lanes) for h in range(cuts)]
    cuts_of = (
        thin[:-1] + [(u * short, short, (cuts - 1) * lanes, lanes) for u in range(2)],
        [(0, short, 0, rows)] + [(short, short, h * lanes, lanes) for h in range(cuts)],
        thin,
    )

    def staged(stage, i, d):
        row, tall_by, column, wide_by = cuts_of[stage][i]
        return stage + 1, slice(row, row + tall_by), pl.ds(pl.multiple_of(d * rows + column, lanes), wide_by)

    def landing(stage, i, by):
        row, tall_by, column, wide_by = cuts_of[stage][i]
        return stage, by, slice(row, row + tall_by), slice(column, column + wide_by)

    def cross(stage, i, d, to, by):
        return remote(
            slots.at[staged(stage, i, d)], crossed.at[landing(stage, i, by)],
            cross_send.at[stage, d, i], cross_recv.at[stage, by, i], (to, d),
        )

    def put(stage, i, d, block, to, keeps=True, later=False):
        def away():
            slots[staged(stage, i, d)] = block
            if not later:
                cross(stage, i, d, to, s).start()

        if keeps:
            pl.when(d != s)(away)

            @pl.when(d == s)
            def _():
                crossed[landing(stage, i, s)] = block
        else:
            away()

    def dispatch(act):
        @pl.loop(0, count)
        def _(k):
            act(peer(k))

    def absorb(stage, waits, use, keeps=True):
        if keeps:
            use(s, True)

        @pl.loop(0, count)
        def _(k):
            d = peer(k)

            def arrive(first):
                for i in waits:
                    cross(stage, i, d, t, d).wait_recv()
                use(d, first)

            if keeps:
                pl.when(d != s)(lambda: arrive(False))
            else:
                pl.when(k == 0)(lambda: arrive(True))
                pl.when(k != 0)(lambda: arrive(False))

    def left_rows(start_row, size, h):
        lines, columns = at(start_row, size), slice(h * lanes, (h + 1) * lanes)
        return dot3((basis[0, lines, :], basis[1, lines, :]), (tall[0, :, columns], tall[1, :, columns]))

    def rows_into(ref, stage, lines):
        def use(d, first):
            block = halves(crossed[stage, d, lines, :])

            @pl.loop(0, 2)
            def _(n):
                columns = at(n * half, half)
                term = dot3(block, (basis_t[0, span(d), columns], basis_t[1, span(d), columns]))
                ref[lines, columns] = term if first else ref[lines, columns] + term
        return use

    for h in range(cuts):
        solve(h)
        if h < cuts - 1:
            dispatch(lambda d: put(0, h, d, left_rows(d * rows, rows, h), t))
        else:
            for u in range(2):
                dispatch(lambda d: put(0, h + u, d, left_rows(d * rows + u * short, short, h), t))

    for u in range(2):
        lines = slice(u * short, (u + 1) * short)
        absorb(0, range(cuts) if u == 0 else [cuts], rows_into(coarse_out, 0, lines))
        moved = jnp.where(t == last, 0.0, reacted(coarse_out[lines, :]))
        halves_to(wide, (lines, slice(None)), moved + fine_next[lines, :])

        def right_part(d):
            block = dot3((wide[0, lines, :], wide[1, lines, :]), (basis[0, :, span(d)], basis[1, :, span(d)]))
            if u == 0:
                put(1, 0, d, block, t)
            else:
                for h in range(cuts):
                    put(1, 1 + h, d, block[:, h * lanes:(h + 1) * lanes], t, later=h > 0)

        dispatch(right_part)

    def send_rest(d):
        @pl.when(d != s)
        def _():
            for h in range(1, cuts):
                cross(1, 1 + h, d, t, s).start()

    dispatch(send_rest)

    for h in range(cuts):
        columns = slice(h * lanes, (h + 1) * lanes)

        def columns_use(d, first):
            block = halves(crossed[1, d, :, columns])

            @pl.loop(0, 2)
            def _(r):
                lines = at(r * half, half)
                term = dot3((basis_t[0, lines, span(d)], basis_t[1, lines, span(d)]), block)
                kept[lines, columns] = term if first else kept[lines, columns] + term

        absorb(1, [0, 1] if h == 0 else [1 + h], columns_use)

        @pl.loop(0, pieces)
        def _(r):
            block = at(r * piece, piece)
            halves_to(tall, (block, columns), kept[block, columns] * fine_decay(block, column_of(h)))

        dispatch(lambda d: put(2, h, d, left_rows(d * rows, rows, h), following, keeps=False))

    absorb(2, range(cuts), rows_into(fine_out, 2, slice(0, rows)), keeps=False)

    @pl.when(holds)
    def _():
        leave_terms(cuts - 1)
        leave_home(coarse, 1)
        leave_home(fine_next, 2)

    leave_home(coarse_next, 3)

    @pl.when(t != last)
    def _():
        pass_guess(0).wait_send()
        pass_guess(1).wait_send()

    pass_fine.wait_send()
    pass_coarse.wait_send()
    for h in range(cuts):
        swap_terms(h).wait_send()
        swap_states(h).wait_send()
        elsewhere(lambda k: share_out(h, k).wait_send())
        elsewhere(lambda k: fan_out(h, k).wait_send())
    for stage, to in ((0, t), (1, t), (2, following)):
        @pl.loop(0, count)
        def _(d):
            def leave():
                for i in range(len(cuts_of[stage])):
                    cross(stage, i, d, to, s).wait_send()

            if stage == 2:
                leave()
            else:
                pl.when(d != s)(leave)


def on_device(initial, guess, fine, coarse, basis, rates, carried):
    grid, rows = basis.shape[0], initial.shape[0]
    half = grid // 2
    piece, count = half // 2, grid // rows
    per_half, pieces = count // 2, grid // piece
    steps, lanes = 7, 128
    cuts = rows // lanes
    pairs = lax.axis_size("tm") // 2
    share = half // pairs
    f32, bf16 = jnp.float32, jnp.bfloat16
    vmem, hbm = pl.BlockSpec(memory_space=pltpu.VMEM), pl.BlockSpec(memory_space=pltpu.HBM)
    dma = pltpu.SemaphoreType.DMA
    fine_new, coarse_new = pl.pallas_call(
        cycle_kernel,
        out_shape=[jax.ShapeDtypeStruct((rows, grid), f32)] * 2,
        in_specs=[hbm] * 6 + [vmem],
        out_specs=[vmem] * 2,
        scratch_shapes=[
            pltpu.VMEM((2, grid, grid), bf16),
            pltpu.VMEM((2, grid, grid), bf16),
            pltpu.VMEM((grid, lanes), f32),
            pltpu.VMEM((rows, grid), f32),
            pltpu.VMEM((rows, grid), f32),
            pltpu.VMEM((rows, grid), f32),
            pltpu.VMEM((rows, grid), f32),
            pltpu.VMEM((rows, grid), f32),
            pltpu.VMEM((4, half, grid), f32),
            pltpu.VMEM((half, grid), f32),
            pltpu.VMEM((grid, half), f32),
            pltpu.VMEM((grid, half), f32),
            pltpu.VMEM((2, half, grid), bf16),
            pltpu.VMEM((2, grid, half), bf16),
            pltpu.VMEM((2, half, half), bf16),
            pltpu.VMEM((2, half, half), f32),
            pltpu.VMEM((2, half, half), f32),
            pltpu.VMEM((grid, half), f32),
            pltpu.VMEM((grid, rows), f32),
            pltpu.VMEM((half, rows), f32),
            pltpu.VMEM((pairs, share, rows), f32),
            pltpu.VMEM((half, rows), f32),
            pltpu.VMEM((half, rows), f32),
            pltpu.VMEM((3, count, rows, rows), f32),
            pltpu.VMEM((share, rows), f32),
            dma((4, 2)),
            dma((4,)),
            dma((4,)),
            dma((4, count)),
            dma((steps, 2)),
            dma((steps, 2)),
            dma((cuts, pieces, per_half)),
            dma((cuts, pieces)),
            dma((2, cuts)),
            dma((2, cuts)),
            dma((2, cuts, pairs)),
            dma((2, cuts, pairs)),
            dma((3, count, cuts + 1)),
            dma((3, count, cuts + 1)),
            dma((5,)),
        ],
        compiler_params=pltpu.CompilerParams(has_side_effects=True, vmem_limit_bytes=50 * 1024 * 1024),
        cost_estimate=pl.CostEstimate(flops=200_000_000_000, bytes_accessed=16 * grid * grid, transcendentals=0),
        name="cycle",
    )(basis, guess[0], initial, fine[0], coarse[0], carried, rates[None, :])
    return fine_new[None], coarse_new[None]


def solution(mesh):
    placed = (
        P("space", None),
        P("tm", "space", None),
        P("tm", "space", None),
        P("tm", "space", None),
        P(),
        P(),
        P(),
    )
    return jax.shard_map(
        on_device,
        mesh=mesh,
        in_specs=placed,
        out_specs=(P("tm", "space", None), P("tm", "space", None)),
        check_vma=False,
    )
```

```python
import functools
import jax
import jax.numpy as jnp
from jax import lax
from jax.experimental import pallas as pl
from jax.experimental.pallas import tpu as pltpu
from jax.sharding import PartitionSpec as P

MESH = pl.DeviceIdType.MESH


def halves(block):
    high = block.astype(jnp.bfloat16)
    return high, (block - high.astype(jnp.float32)).astype(jnp.bfloat16)


def dot3(left, right):
    dot = functools.partial(jnp.dot, preferred_element_type=jnp.float32)
    return dot(left[0], right[0]) + dot(left[0], right[1]) + dot(left[1], right[0])


def reacted(value):
    return value + 0.5 * jnp.tanh(value)


def cycle_kernel(
    raw, guess, initial, fine, coarse, carried, rates, fine_out, coarse_out,
    basis, basis_t, rates_tall, fine_here, before, entry, fine_next, coarse_next, slots, field, coeffs, kept, wide, tall, part,
    sent, held, decay, landed, gathered, evens, got, crossed, start,
    home_send, shift_send, shift_recv, slot_recv, ex_send, ex_recv, term_send, term_recv,
    pair_send, pair_recv, share_send, share_recv, cross_send, cross_recv, load_sem,
):
    groups, count = lax.axis_size("tm"), lax.axis_size("space")
    t, s = lax.axis_index("tm"), lax.axis_index("space")
    grid = raw.shape[0]
    rows = fine_here.shape[0]
    short = rows // 2
    half = grid // 2
    piece = half // 2
    pieces = grid // piece
    per_half = count // 2
    low_seat = per_half - 1
    last = groups - 1
    lanes = rates_tall.shape[1]
    cuts = rows // lanes
    pairs = groups // 2
    share = half // pairs

    def at(start, size):
        return pl.ds(pl.multiple_of(start, size), size)

    def span(d):
        return at(d * rows, rows)

    def seat(chain):
        return low_seat + chain % 2

    def core(chain, which):
        return 2 * (chain // 2) + which

    def remote(src, dst, send, recv, where):
        return pltpu.make_async_remote_copy(
            src_ref=src, dst_ref=dst, send_sem=send, recv_sem=recv,
            device_id={"tm": where[0], "space": where[1]}, device_id_type=MESH,
        )

    position = s % per_half
    group_at = (core(t, s // per_half), seat(t))
    to_self = (group_at[0] == t) & (group_at[1] == s)
    following, preceding = (t + 1) % groups, (t + groups - 1) % groups

    def group_copy(src, slot, k):
        part_of = src.at[at(k * short, short)]
        dst = slots.at[slot, at(position * rows + k * short, short)]
        return part_of, dst, home_send.at[slot, k], slot_recv.at[slot, 2 * position + k]

    def to_group(src, slot, k):
        part_of, dst, send, recv = group_copy(src, slot, k)

        @pl.when(jnp.logical_not(to_self))
        def _():
            remote(part_of, dst, send, recv, group_at).start()

        @pl.when(to_self)
        def _():
            pltpu.make_async_copy(part_of, dst, recv).start()

    def leave_home(src, slot):
        @pl.when(jnp.logical_not(to_self))
        def _():
            for k in range(2):
                remote(*group_copy(src, slot, k), group_at).wait_send()

    def pass_on(index, src, dst, where):
        return remote(src, dst, shift_send.at[index], shift_recv.at[index], (where, s))

    def pass_guess(k):
        lines = at(k * short, short)
        return pass_on(k, guess.at[lines], before.at[lines], following)

    pass_fine = pass_on(2, fine, fine_next, preceding)
    pass_entry = pass_on(2, entry, fine_next, preceding)
    pass_coarse = pass_on(3, coarse, coarse_next, preceding)

    side = t % 2
    pair = t // 2
    own, other = at(side * half, half), at((1 - side) * half, half)
    partner = (core(t, 1 - side), s)
    start_copy = pltpu.make_async_copy(
        carried.at[at(side * half + pair * share, share), span(s)], start, load_sem.at[0]
    )
    load_fine = pltpu.make_async_copy(fine, fine_here, load_sem.at[1])
    load_initial = pltpu.make_async_copy(initial, before, load_sem.at[2])
    load_low = pltpu.make_async_copy(raw.at[:, 0:half], coeffs, load_sem.at[3])
    load_high = pltpu.make_async_copy(raw.at[:, half:grid], kept, load_sem.at[4])

    @pl.when(t != last)
    def _():
        pass_guess(0).start()
        pass_guess(1).start()

    load_fine.start()

    @pl.when(t == 0)
    def _():
        load_initial.start()

    load_low.start()
    load_high.start()
    start_copy.start()

    @pl.when(t % 2 == 0)
    def _():
        to_group(coarse, 1, 0)

    load_fine.wait()

    @pl.when(t == 0)
    def _():
        load_initial.wait()

    for k in range(2):
        @pl.when(t != 0)
        def _():
            pass_guess(k).wait_recv()

        lines = at(k * short, short)
        entry[lines, :] = reacted(before[lines, :]) + fine_here[lines, :]
        to_group(entry, 0, k)

    @pl.when(t != 0)
    def _():
        pass_fine.start()

    load_low.wait()
    load_high.wait()
    for which, ref in enumerate((coeffs, kept)):
        @pl.loop(0, count)
        def _(r):
            high, low = halves(ref[span(r), :])
            basis[0, span(r), which * half:(which + 1) * half] = high
            basis[1, span(r), which * half:(which + 1) * half] = low

        @pl.loop(0, pieces)
        def _(c):
            for r in range(2):
                lines = slice(which * half + r * piece, which * half + (r + 1) * piece)
                high, low = halves(ref[at(c * piece, piece), r * piece:(r + 1) * piece].T)
                basis_t[0, lines, at(c * piece, piece)] = high
                basis_t[1, lines, at(c * piece, piece)] = low

    @pl.loop(0, grid // lanes)
    def _(r):
        rates_tall[at(r * lanes, lanes), :] = jnp.broadcast_to(rates[:, at(r * lanes, lanes)], (lanes, lanes)).T

    leave_home(entry, 0)

    @pl.when(t == 0)
    def _():
        pass_entry.start()

    @pl.when(t % 2 == 1)
    def _():
        to_group(coarse, 1, 0)

    to_group(coarse, 1, 1)
    pass_coarse.start()

    def home_fine():
        pass_fine.wait_recv()
        to_group(fine_next, 2, 0)
        to_group(fine_next, 2, 1)

    def home_coarse():
        pass_coarse.wait_recv()
        to_group(coarse_next, 3, 0)
        to_group(coarse_next, 3, 1)

    def sums_of_rates(block, columns):
        return rates_tall[block, :1] + rates[:, columns]

    def fine_decay(block, columns):
        return 1.0 / (1.0 + sums_of_rates(block, columns))

    def coarse_decay(block, columns):
        return 1.0 / (1.0 + 2.0 * sums_of_rates(block, columns))

    group = core(t, s - low_seat)

    def wait_slot(slot, index):
        local = (group == t) & (side * per_half + index == s)
        for k in range(2):
            dst = slots.at[slot, at(index * rows + k * short, short)]
            src, recv = entry.at[at(k * short, short)], slot_recv.at[slot, 2 * index + k]

            @pl.when(jnp.logical_not(local))
            def _():
                remote(src, dst, home_send.at[slot, k], recv, (t, s)).wait_recv()

            @pl.when(local)
            def _():
                pltpu.make_async_copy(src, dst, recv).wait()

    def exchange(stage, m):
        block = at(m * piece, piece)
        return remote(sent.at[stage % 2, block], held.at[stage % 2, block], ex_send.at[stage, m], ex_recv.at[stage, m], partner)

    def halves_to(ref, index, value):
        ref[(0, *index)], ref[(1, *index)] = halves(value)

    def reorder(value, order):
        if not order:
            return value
        return jnp.concatenate(
            [value[:, q * rows + h * lanes:q * rows + (h + 1) * lanes] for h in range(cuts) for q in range(per_half)], 1
        )

    def collect(stage, into, order=False):
        for m in range(2):
            block = at(m * piece, piece)
            exchange(stage, m).wait_recv()
            halves_to(into, (block, slice(0, half)), reorder(held[stage % 2, block, :], order))

    def free(stage):
        if stage >= 2:
            for m in range(2):
                exchange(stage - 2, m).wait_send()

    def right_of(stage, source, slot, order=False):
        free(stage)
        for m in range(2):
            block = at(m * piece, piece)
            for index in range(m * per_half // 2, (m + 1) * per_half // 2):
                wait_slot(slot, index)
            halves_to(wide, (block, slice(None)), source(block))
            left = (wide[0, block, :], wide[1, block, :])
            sent[stage % 2, block] = dot3(left, (basis[0, :, other], basis[1, :, other]))
            exchange(stage, m).start()
            halves_to(part, (block, slice(None)), reorder(dot3(left, (basis[0, :, own], basis[1, :, own])), order))

    def forward(stage, source, slot, finish):
        right_of(stage, source, slot)

        @pl.loop(0, 2)
        def _(n):
            columns = at(n * piece, piece)
            coeffs[:, columns] = dot3((basis_t[0, :, own], basis_t[1, :, own]), (part[0, :, columns], part[1, :, columns]))

        collect(stage, part)

        @pl.loop(0, 2)
        def _(n):
            columns = at(n * piece, piece)
            term = dot3((basis_t[0, :, other], basis_t[1, :, other]), (part[0, :, columns], part[1, :, columns]))
            value = (coeffs[:, columns] + term) * decay[:, columns]
            coeffs[:, columns] = value
            finish(n, columns, value)

    def inverse(stage, midway=None):
        free(stage)

        @pl.loop(0, pieces)
        def _(r):
            block = at(r * piece, piece)
            halves_to(tall, (block, slice(None)), coeffs[block, :])

        def rows_of(m, which):
            block = at(which * half + m * piece, piece)
            return dot3((basis[0, block, :], basis[1, block, :]), (tall[0], tall[1]))

        @pl.loop(0, 2)
        def _(m):
            sent[stage % 2, at(m * piece, piece)] = rows_of(m, 1 - side)
            exchange(stage, m).start()

        @pl.loop(0, 2)
        def _(m):
            halves_to(part, (at(m * piece, piece), slice(None)), rows_of(m, side))

        if midway is not None:
            midway()

        @pl.loop(0, 2)
        def _(n):
            columns = at(n * half, half)
            field[:, columns] = dot3((part[0], part[1]), (basis_t[0, own, columns], basis_t[1, own, columns]))

        collect(stage, part)

        @pl.loop(0, 2)
        def _(n):
            columns = at(n * half, half)
            field[:, columns] = field[:, columns] + dot3(
                (part[0], part[1]), (basis_t[0, other, columns], basis_t[1, other, columns])
            )

    def term_place(r, q):
        return core(group, r // 2), side * per_half + q

    def term_refs(h, r, q, parity):
        source = coeffs.at[at(r * piece, piece), at((h * per_half + q) * lanes, lanes)]
        target = landed.at[parity, at((r % 2) * piece, piece), at(h * lanes, lanes)]
        return source, target, term_recv.at[h, 2 * parity + r % 2]

    def term_here(r, q):
        where = term_place(r, q)
        return (where[0] == t) & (where[1] == s)

    def term_copy(h, r, q):
        source, target, recv = term_refs(h, r, q, group % 2)
        return remote(source, target, term_send.at[h, r, q], recv, term_place(r, q))

    def send_term(h, r, q):
        @pl.when(term_here(r, q))
        def _():
            pltpu.make_async_copy(*term_refs(h, r, q, group % 2)).start()

        @pl.when(jnp.logical_not(term_here(r, q)))
        def _():
            term_copy(h, r, q).start()

    def leave_terms(h):
        for r in range(pieces):
            for q in range(per_half):
                @pl.when(jnp.logical_not(term_here(r, q)))
                def _():
                    term_copy(h, r, q).wait_send()

    holds = (s == low_seat) | (s == low_seat + 1)

    @pl.when(jnp.logical_not(holds))
    def _():
        leave_home(coarse, 1)
        home_fine()
        leave_home(fine_next, 2)
        home_coarse()

    @pl.when(holds)
    def _():
        @pl.loop(0, pieces)
        def _(r):
            block = at(r * piece, piece)
            decay[block, :] = fine_decay(block, own)

        def plain(n, columns, value):
            pass

        def keep(n, columns, value):
            taken = value * coarse_decay(slice(None), at(side * half + n * piece, piece))
            kept[:, columns] = jnp.where(group == last, 0.0, taken)

        def from_field(slot):
            def source(block):
                moved = reacted(field[block, :])
                if slot == 2:
                    moved = jnp.where(group == last, 0.0, moved)
                return moved + slots[slot, block, :]
            return source

        forward(0, lambda block: slots[0, block, :], 0, plain)
        home_fine()
        inverse(1)
        forward(2, from_field(1), 1, keep)
        inverse(3, home_coarse)
        forward(4, from_field(2), 2, plain)
        inverse(5)

        right_of(6, from_field(3), 3, True)
        collect(6, wide, True)
        for h in range(cuts):
            columns = slice(h * per_half * lanes, (h + 1) * per_half * lanes)

            @pl.loop(0, pieces)
            def _(r):
                block = at(r * piece, piece)
                value = dot3((basis_t[0, block, own], basis_t[1, block, own]), (part[0, :, columns], part[1, :, columns]))
                value = value + dot3(
                    (basis_t[0, block, other], basis_t[1, block, other]), (wide[0, :, columns], wide[1, :, columns])
                )
                for q in range(per_half):
                    natural = slice(q * rows + h * lanes, q * rows + (h + 1) * lanes)
                    coeffs[block, at((h * per_half + q) * lanes, lanes)] = (
                        value[:, q * lanes:(q + 1) * lanes] * decay[block, natural] - kept[block, natural]
                    )
                if h == 0:
                    for q in range(per_half):
                        send_term(h, r, q)

            if h > 0:
                leave_terms(h - 1)
                for r in range(pieces):
                    for q in range(per_half):
                        send_term(h, r, q)

        for stage in (5, 6):
            for m in range(2):
                exchange(stage, m).wait_send()

    def wait_term(h, parity, k):
        member = core(t, parity)
        from_self = (core(t, s // per_half) == t) & (seat(member) == s)
        source, target, recv = term_refs(h, k, 0, parity)

        @pl.when(from_self)
        def _():
            pltpu.make_async_copy(source, target, recv).wait()

        @pl.when(jnp.logical_not(from_self))
        def _():
            remote(source, target, term_send.at[h, k, 0], recv, (t, s)).wait_recv()

    spread, fanned, given = (slots.at[0, :, at(k * rows, rows)] for k in range(3))

    def cut(h):
        return at(h * lanes, lanes)

    def column_of(h):
        return at(s * rows + h * lanes, lanes)

    def swap_states(h):
        return remote(given.at[:, cut(h)], got.at[:, cut(h)], pair_send.at[h], pair_recv.at[h], partner)

    def share_out(h, k):
        return remote(
            spread.at[at(k * share, share), cut(h)], gathered.at[pair, :, cut(h)],
            share_send.at[0, h, k], share_recv.at[0, h, pair], (core(2 * k, side), s),
        )

    def share_in(h, k):
        return remote(
            spread.at[at(k * share, share), cut(h)], gathered.at[k, :, cut(h)],
            share_send.at[0, h, k], share_recv.at[0, h, k], (core(2 * k, side), s),
        )

    def fan_out(h, k):
        return remote(
            fanned.at[at(k * share, share), cut(h)], evens.at[at(pair * share, share), cut(h)],
            share_send.at[1, h, k], share_recv.at[1, h, pair], (core(2 * k, side), s),
        )

    def fan_in(h, k):
        return remote(
            fanned.at[at(k * share, share), cut(h)], evens.at[at(k * share, share), cut(h)],
            share_send.at[1, h, k], share_recv.at[1, h, k], (core(2 * k, side), s),
        )

    def elsewhere(act):
        @pl.loop(0, pairs)
        def _(k):
            @pl.when(k != pair)
            def _():
                act(k)

    def open_solve(h):
        rate = coarse_decay(own, column_of(h))
        for parity in range(2):
            for k in range(2):
                wait_term(h, parity, k)
        first, second = landed[0, :, cut(h)], landed[1, :, cut(h)]
        spread[:, cut(h)] = second + jnp.where(pair == pairs - 1, 0.0, rate * first)
        elsewhere(lambda k: share_out(h, k).start())
        gathered[pair, :, cut(h)] = spread[at(pair * share, share), cut(h)]

    def close_solve(h):
        first, rate = landed[0, :, cut(h)], coarse_decay(own, column_of(h))
        if h == 0:
            start_copy.wait()
        elsewhere(lambda k: share_in(h, k).wait_recv())
        near = coarse_decay(at(side * half + pair * share, share), column_of(h))
        value = gathered[pairs - 1, :, cut(h)] + near * start[:, cut(h)]
        fanned[0:share, cut(h)] = value
        near = near * near
        for k in range(pairs - 1):
            value = gathered[k, :, cut(h)] + near * value
            fanned[(k + 1) * share:(k + 2) * share, cut(h)] = value
        elsewhere(lambda k: fan_out(h, k).start())
        evens[at(pair * share, share), cut(h)] = fanned[at(pair * share, share), cut(h)]
        elsewhere(lambda k: fan_in(h, k).wait_recv())
        even = evens[:, cut(h)]
        odd = first + rate * even
        given[:, cut(h)] = jnp.where(side == 0, odd, even)
        swap_states(h).start()
        halves_to(tall, (own, cut(h)), jnp.where(side == 0, even, odd))
        swap_states(h).wait_recv()
        halves_to(tall, (other, cut(h)), got[:, cut(h)])

    def peer(k):
        return jnp.where(s < count // 2, count - 1 - k, k)

    thin = [(0, rows, h * lanes, lanes) for h in range(cuts)]
    cuts_of = (
        thin[:-1] + [(u * short, short, (cuts - 1) * lanes, lanes) for u in range(2)],
        [(0, short, 0, rows)] + [(short, short, h * lanes, lanes) for h in range(cuts)],
        thin,
    )

    def staged(stage, i, d):
        row, tall_by, column, wide_by = cuts_of[stage][i]
        return stage + 1, slice(row, row + tall_by), pl.ds(pl.multiple_of(d * rows + column, lanes), wide_by)

    def landing(stage, i, by):
        row, tall_by, column, wide_by = cuts_of[stage][i]
        return stage, by, slice(row, row + tall_by), slice(column, column + wide_by)

    def cross(stage, i, d, to, by):
        return remote(
            slots.at[staged(stage, i, d)], crossed.at[landing(stage, i, by)],
            cross_send.at[stage, d, i], cross_recv.at[stage, by, i], (to, d),
        )

    def put(stage, i, d, block, to, keeps=True, later=False):
        def away():
            slots[staged(stage, i, d)] = block
            if not later:
                cross(stage, i, d, to, s).start()

        if keeps:
            pl.when(d != s)(away)

            @pl.when(d == s)
            def _():
                crossed[landing(stage, i, s)] = block
        else:
            away()

    def dispatch(act):
        @pl.loop(0, count)
        def _(k):
            act(peer(k))

    def absorb(stage, waits, use, keeps=True):
        if keeps:
            use(s, True)

        @pl.loop(0, count)
        def _(k):
            d = peer(k)

            def arrive(first):
                for i in waits:
                    cross(stage, i, d, t, d).wait_recv()
                use(d, first)

            if keeps:
                pl.when(d != s)(lambda: arrive(False))
            else:
                pl.when(k == 0)(lambda: arrive(True))
                pl.when(k != 0)(lambda: arrive(False))

    def left_rows(start_row, size, h):
        lines, columns = at(start_row, size), slice(h * lanes, (h + 1) * lanes)
        return dot3((basis[0, lines, :], basis[1, lines, :]), (tall[0, :, columns], tall[1, :, columns]))

    def rows_into(ref, stage, lines):
        def use(d, first):
            block = halves(crossed[stage, d, lines, :])

            @pl.loop(0, 2)
            def _(n):
                columns = at(n * half, half)
                term = dot3(block, (basis_t[0, span(d), columns], basis_t[1, span(d), columns]))
                ref[lines, columns] = term if first else ref[lines, columns] + term
        return use

    open_solve(0)
    for h in range(cuts):
        close_solve(h)
        if h < cuts - 1:
            open_solve(h + 1)
            dispatch(lambda d: put(0, h, d, left_rows(d * rows, rows, h), t))
        else:
            for u in range(2):
                dispatch(lambda d: put(0, h + u, d, left_rows(d * rows + u * short, short, h), t))

    for u in range(2):
        lines = slice(u * short, (u + 1) * short)
        absorb(0, range(cuts) if u == 0 else [cuts], rows_into(coarse_out, 0, lines))
        moved = jnp.where(t == last, 0.0, reacted(coarse_out[lines, :]))
        halves_to(wide, (lines, slice(None)), moved + fine_next[lines, :])

        def right_part(d):
            block = dot3((wide[0, lines, :], wide[1, lines, :]), (basis[0, :, span(d)], basis[1, :, span(d)]))
            if u == 0:
                put(1, 0, d, block, t)
            else:
                for h in range(cuts):
                    put(1, 1 + h, d, block[:, h * lanes:(h + 1) * lanes], t, later=h > 0)

        dispatch(right_part)

    def send_rest(d):
        @pl.when(d != s)
        def _():
            for h in range(1, cuts):
                cross(1, 1 + h, d, t, s).start()

    dispatch(send_rest)

    for h in range(cuts):
        columns = slice(h * lanes, (h + 1) * lanes)

        def columns_use(d, first):
            block = halves(crossed[1, d, :, columns])

            @pl.loop(0, 2)
            def _(r):
                lines = at(r * half, half)
                term = dot3((basis_t[0, lines, span(d)], basis_t[1, lines, span(d)]), block)
                kept[lines, columns] = term if first else kept[lines, columns] + term

        absorb(1, [0, 1] if h == 0 else [1 + h], columns_use)

        @pl.loop(0, pieces)
        def _(r):
            block = at(r * piece, piece)
            halves_to(tall, (block, columns), kept[block, columns] * fine_decay(block, column_of(h)))

        dispatch(lambda d: put(2, h, d, left_rows(d * rows, rows, h), following, keeps=False))

    absorb(2, range(cuts), rows_into(fine_out, 2, slice(0, rows)), keeps=False)

    @pl.when(holds)
    def _():
        leave_terms(cuts - 1)
        leave_home(coarse, 1)
        leave_home(fine_next, 2)

    leave_home(coarse_next, 3)

    @pl.when(t != last)
    def _():
        pass_guess(0).wait_send()
        pass_guess(1).wait_send()

    pass_fine.wait_send()
    pass_coarse.wait_send()
    for h in range(cuts):
        swap_states(h).wait_send()
        elsewhere(lambda k: share_out(h, k).wait_send())
        elsewhere(lambda k: fan_out(h, k).wait_send())
    for stage, to in ((0, t), (1, t), (2, following)):
        @pl.loop(0, count)
        def _(d):
            def leave():
                for i in range(len(cuts_of[stage])):
                    cross(stage, i, d, to, s).wait_send()

            if stage == 2:
                leave()
            else:
                pl.when(d != s)(leave)


def on_device(initial, guess, fine, coarse, basis, rates, carried):
    grid, rows = basis.shape[0], initial.shape[0]
    half = grid // 2
    piece, count = half // 2, grid // rows
    per_half, pieces = count // 2, grid // piece
    steps, lanes = 7, 128
    cuts = rows // lanes
    pairs = lax.axis_size("tm") // 2
    share = half // pairs
    f32, bf16 = jnp.float32, jnp.bfloat16
    vmem, hbm = pl.BlockSpec(memory_space=pltpu.VMEM), pl.BlockSpec(memory_space=pltpu.HBM)
    dma = pltpu.SemaphoreType.DMA
    fine_new, coarse_new = pl.pallas_call(
        cycle_kernel,
        out_shape=[jax.ShapeDtypeStruct((rows, grid), f32)] * 2,
        in_specs=[hbm] * 6 + [vmem],
        out_specs=[vmem] * 2,
        scratch_shapes=[
            pltpu.VMEM((2, grid, grid), bf16),
            pltpu.VMEM((2, grid, grid), bf16),
            pltpu.VMEM((grid, lanes), f32),
            pltpu.VMEM((rows, grid), f32),
            pltpu.VMEM((rows, grid), f32),
            pltpu.VMEM((rows, grid), f32),
            pltpu.VMEM((rows, grid), f32),
            pltpu.VMEM((rows, grid), f32),
            pltpu.VMEM((4, half, grid), f32),
            pltpu.VMEM((half, grid), f32),
            pltpu.VMEM((grid, half), f32),
            pltpu.VMEM((grid, half), f32),
            pltpu.VMEM((2, half, grid), bf16),
            pltpu.VMEM((2, grid, half), bf16),
            pltpu.VMEM((2, half, half), bf16),
            pltpu.VMEM((2, half, half), f32),
            pltpu.VMEM((2, half, half), f32),
            pltpu.VMEM((grid, half), f32),
            pltpu.VMEM((2, half, rows), f32),
            pltpu.VMEM((pairs, share, rows), f32),
            pltpu.VMEM((half, rows), f32),
            pltpu.VMEM((half, rows), f32),
            pltpu.VMEM((3, count, rows, rows), f32),
            pltpu.VMEM((share, rows), f32),
            dma((4, 2)),
            dma((4,)),
            dma((4,)),
            dma((4, count)),
            dma((steps, 2)),
            dma((steps, 2)),
            dma((cuts, pieces, per_half)),
            dma((cuts, pieces)),
            dma((cuts,)),
            dma((cuts,)),
            dma((2, cuts, pairs)),
            dma((2, cuts, pairs)),
            dma((3, count, cuts + 1)),
            dma((3, count, cuts + 1)),
            dma((5,)),
        ],
        compiler_params=pltpu.CompilerParams(has_side_effects=True, vmem_limit_bytes=50 * 1024 * 1024),
        cost_estimate=pl.CostEstimate(flops=200_000_000_000, bytes_accessed=16 * grid * grid, transcendentals=0),
        name="cycle",
    )(basis, guess[0], initial, fine[0], coarse[0], carried, rates[None, :])
    return fine_new[None], coarse_new[None]


def solution(mesh):
    placed = (
        P("space", None),
        P("tm", "space", None),
        P("tm", "space", None),
        P("tm", "space", None),
        P(),
        P(),
        P(),
    )
    return jax.shard_map(
        on_device,
        mesh=mesh,
        in_specs=placed,
        out_specs=(P("tm", "space", None), P("tm", "space", None)),
        check_vma=False,
    )
```
